8 devices in a mesh: dp: 1 (over z), tp: 8 (over y, x, core).
Axes of the slice: x: 2, y: 2, z: 1, core: 2. Of those that a mesh axis runs over, the one named last changes fastest.
Arguments:
- x_in: bfloat16 [1536, 3072], P(('dp', 'tp'))
- grad_y: bfloat16 [1536, 3072], P(('dp', 'tp'))
- norm_gain: float32 [3, 3072], replicated
- w_qkv: bfloat16 [3, 3072, 5120], P(None, None, 'tp')
- w_out: bfloat16 [3, 3072, 3072], P(None, 'tp')
- w_gate: bfloat16 [3, 3072, 8192], P(None, None, 'tp')
- w_up: bfloat16 [3, 3072, 8192], P(None, None, 'tp')
- w_down: bfloat16 [3, 8192, 3072], P(None, 'tp')
Outputs:
- output 1: bfloat16 [1536, 3072], P(('dp', 'tp'))
- output 2: float32 [3, 3072], P('dp')
- output 3: bfloat16 [3, 3072, 5120], P('dp', None, 'tp')
- output 4: bfloat16 [3, 3072, 3072], P('dp', 'tp')
- output 5: bfloat16 [3, 3072, 8192], P('dp', None, 'tp')
- output 6: bfloat16 [3, 3072, 8192], P('dp', None, 'tp')
- output 7: bfloat16 [3, 8192, 3072], P('dp', 'tp')
All inputs are finite; a program needn't handle non-finite values.
Results may differ from the reference program's by a relative error of at most 0.02.
Values are sent between devices in bfloat16 or wider.
A program may use at most 1 GiB of HBM per device.

```python
import jax
import jax.numpy as jnp
from jax import lax

SEQ_LEN = 1536
D_MODEL = 3072
D_FF = 8192
HEADS = 24
KV_HEADS = 8
HEAD_DIM = 128
LAYERS = 3

GROUP_SIZE = HEADS // KV_HEADS
QKV_COLS = (HEADS + 2 * KV_HEADS) * HEAD_DIM
NORM_EPS = 1e-5
ROPE_BASE = 10000.0


def setup_inputs(seed: int = 0, part: int = 0) -> dict:
    data_keys = jax.random.split(jax.random.fold_in(jax.random.key(seed), part), 2)
    weight_keys = jax.random.split(jax.random.key(seed + 1), 6)
    x_in = jax.random.normal(data_keys[0], (SEQ_LEN, D_MODEL), jnp.float32)
    grad_y = jax.random.normal(data_keys[1], (SEQ_LEN, D_MODEL), jnp.float32)
    norm_gain = 1.0 + 0.3 * jax.random.normal(weight_keys[0], (LAYERS, D_MODEL), jnp.float32)
    w_qkv = jax.random.normal(weight_keys[1], (LAYERS, D_MODEL, QKV_COLS), jnp.float32) * D_MODEL ** -0.5
    w_out = jax.random.normal(weight_keys[2], (LAYERS, HEADS * HEAD_DIM, D_MODEL), jnp.float32) * (HEADS * HEAD_DIM) ** -0.5
    w_gate = jax.random.normal(weight_keys[3], (LAYERS, D_MODEL, D_FF), jnp.float32) * D_MODEL ** -0.5
    w_up = jax.random.normal(weight_keys[4], (LAYERS, D_MODEL, D_FF), jnp.float32) * D_MODEL ** -0.5
    w_down = jax.random.normal(weight_keys[5], (LAYERS, D_FF, D_MODEL), jnp.float32) * D_FF ** -0.5
    return {'x_in': x_in.astype(jnp.bfloat16), 'grad_y': grad_y.astype(jnp.bfloat16), 'norm_gain': norm_gain, 'w_qkv': w_qkv.astype(jnp.bfloat16), 'w_out': w_out.astype(jnp.bfloat16), 'w_gate': w_gate.astype(jnp.bfloat16), 'w_up': w_up.astype(jnp.bfloat16), 'w_down': w_down.astype(jnp.bfloat16)}


def rope_tables():
    half_dim = HEAD_DIM // 2
    freqs = ROPE_BASE ** (-2.0 * jnp.arange(half_dim, dtype=jnp.float32) / HEAD_DIM)
    angles = jnp.arange(SEQ_LEN, dtype=jnp.float32)[:, None] * freqs[None, :]
    return jnp.cos(angles)[:, None, None, :], jnp.sin(angles)[:, None, None, :]


def rotate(values, cos_tab, sin_tab):
    half_dim = values.shape[-1] // 2
    lower_half = values[..., :half_dim]
    upper_half = values[..., half_dim:]
    return jnp.concatenate([lower_half * cos_tab - upper_half * sin_tab, upper_half * cos_tab + lower_half * sin_tab], axis=-1)


def rms_scale(x_f32, gain_row):
    inv_rms = lax.rsqrt(jnp.mean(x_f32 * x_f32, axis=-1, keepdims=True) + NORM_EPS)
    return x_f32 * inv_rms * gain_row


def group_attention(operands):
    query, keys_rot, values_v = operands
    causal = jnp.arange(SEQ_LEN)[:, None] >= jnp.arange(SEQ_LEN)[None, :]
    scores = jnp.einsum('sgd,td->gst', query.astype(jnp.float32), keys_rot.astype(jnp.float32)) * HEAD_DIM ** -0.5
    attn_prob = jax.nn.softmax(jnp.where(causal, scores, -1e30), axis=-1).astype(jnp.bfloat16)
    return jnp.einsum('gst,td->sgd', attn_prob.astype(jnp.float32), values_v.astype(jnp.float32)).astype(jnp.bfloat16)


def decoder_block(x_cur, gain_row, w_qkv_l, w_out_l, w_gate_l, w_up_l, w_down_l, cos_tab, sin_tab):
    x_f32 = x_cur.astype(jnp.float32)
    normed = rms_scale(x_f32, gain_row).astype(jnp.bfloat16).astype(jnp.float32)
    qkv_all = jnp.dot(normed, w_qkv_l.astype(jnp.float32), preferred_element_type=jnp.float32).astype(jnp.bfloat16)
    qkv_all = qkv_all.reshape(SEQ_LEN, KV_HEADS, GROUP_SIZE + 2, HEAD_DIM)
    rotated = rotate(qkv_all[:, :, :GROUP_SIZE + 1].astype(jnp.float32), cos_tab, sin_tab).astype(jnp.bfloat16)
    operands = (jnp.moveaxis(rotated[:, :, :GROUP_SIZE], 1, 0), jnp.moveaxis(rotated[:, :, GROUP_SIZE], 1, 0), jnp.moveaxis(qkv_all[:, :, GROUP_SIZE + 1], 1, 0))
    attn_out = lax.map(jax.checkpoint(group_attention), operands)
    attn_out = jnp.moveaxis(attn_out, 0, 1).reshape(SEQ_LEN, HEADS * HEAD_DIM)
    gate_act = jnp.dot(normed, w_gate_l.astype(jnp.float32), preferred_element_type=jnp.float32).astype(jnp.bfloat16)
    up_act = jnp.dot(normed, w_up_l.astype(jnp.float32), preferred_element_type=jnp.float32).astype(jnp.bfloat16)
    hidden = (jax.nn.silu(gate_act.astype(jnp.float32)) * up_act.astype(jnp.float32)).astype(jnp.bfloat16)
    block_sum = x_f32 + jnp.dot(attn_out.astype(jnp.float32), w_out_l.astype(jnp.float32), preferred_element_type=jnp.float32) + jnp.dot(hidden.astype(jnp.float32), w_down_l.astype(jnp.float32), preferred_element_type=jnp.float32)
    return block_sum.astype(jnp.bfloat16)


def stack_forward(x_in, norm_gain, w_qkv, w_out, w_gate, w_up, w_down):
    cos_tab, sin_tab = rope_tables()

    def body(x_cur, layer_weights):
        gain_row, w_qkv_l, w_out_l, w_gate_l, w_up_l, w_down_l = layer_weights
        return decoder_block(x_cur, gain_row, w_qkv_l, w_out_l, w_gate_l, w_up_l, w_down_l, cos_tab, sin_tab), None

    return lax.scan(body, x_in, (norm_gain, w_qkv, w_out, w_gate, w_up, w_down))[0]


def reference(x_in, grad_y, norm_gain, w_qkv, w_out, w_gate, w_up, w_down):
    pullback = jax.vjp(stack_forward, x_in, norm_gain, w_qkv, w_out, w_gate, w_up, w_down)[1]
    grad_x, grad_gain, grad_qkv, grad_out, grad_gate, grad_up, grad_down = pullback(grad_y)
    return (grad_x, grad_gain, grad_qkv, grad_out, grad_gate, grad_up, grad_down)
```

```python
import functools

import jax
import jax.numpy as jnp
from jax import lax
from jax.experimental import pallas as pl
from jax.experimental.pallas import tpu as pltpu
from jax.sharding import PartitionSpec as P

HEAD_DIM = 128
NORM_EPS = 1e-5
ROPE_BASE = 10000.0
BF16 = jnp.bfloat16
F32 = jnp.float32
VMEM_MAX = 67043328


def rope_tables(seq_len):
    half_dim = HEAD_DIM // 2
    freqs = ROPE_BASE ** (-2.0 * jnp.arange(half_dim, dtype=F32) / HEAD_DIM)
    angles = jnp.arange(seq_len, dtype=F32)[:, None] * freqs[None, :]
    cos, sin = jnp.cos(angles), jnp.sin(angles)
    return jnp.concatenate([cos, cos], axis=1), jnp.concatenate([-sin, sin], axis=1)


def rms_scale(x_f32, gain_row):
    inv_rms = lax.rsqrt(jnp.mean(x_f32 * x_f32, axis=-1, keepdims=True) + NORM_EPS)
    return x_f32 * inv_rms * gain_row


def gated(gate_f32, up_f32):
    return jax.nn.silu(gate_f32) * up_f32


def dot_nt(lhs, rhs):
    return lax.dot_general(lhs, rhs, (((1,), (1,)), ((), ())), preferred_element_type=F32)


def dot_tn(lhs, rhs):
    return lax.dot_general(lhs, rhs, (((0,), (0,)), ((), ())), preferred_element_type=F32)


def dot_nn(lhs, rhs):
    return lax.dot_general(lhs, rhs, (((1,), (0,)), ((), ())), preferred_element_type=F32)


def turn(values, cos_tab, sin_tab):
    return values * cos_tab + pltpu.roll(values, HEAD_DIM // 2, 1) * sin_tab


def attn_fwd_body(heads, blk, qkv_ref, cos_ref, sin_ref, kv_ref, q_out, k_out, o_out, lse_out, score_buf, k_rot):
    step = pl.program_id(0)
    scale = HEAD_DIM ** -0.5
    kcol = heads * HEAD_DIM
    vcol = kcol + HEAD_DIM
    cos_tab, sin_tab = cos_ref[...], sin_ref[...]
    here = pl.ds(pl.multiple_of(step * blk, blk), blk)
    key = turn(qkv_ref[:, kcol:vcol].astype(F32), cos_tab, sin_tab).astype(BF16)
    k_rot[here, :] = key
    k_out[...] = key
    parts = []
    for head in range(heads):
        cols = slice(head * HEAD_DIM, (head + 1) * HEAD_DIM)
        part = turn(qkv_ref[:, cols].astype(F32), cos_tab, sin_tab).astype(BF16)
        q_out[:, cols] = part
        parts.append(part)
    query = jnp.concatenate(parts, axis=0)
    rows = heads * blk

    diag = dot_nt(query, key) * scale
    row_id = lax.broadcasted_iota(jnp.int32, (heads, blk, blk), 1).reshape(rows, blk)
    col_id = lax.broadcasted_iota(jnp.int32, (rows, blk), 1)
    diag = jnp.where(row_id >= col_id, diag, -1e30)
    top = jnp.max(diag, axis=-1, keepdims=True)

    def first(j, top):
        there = pl.ds(pl.multiple_of(j * blk, blk), blk)
        score = dot_nt(query, k_rot[there, :]) * scale
        score_buf[j] = score
        return jnp.maximum(top, jnp.max(score, axis=-1, keepdims=True))

    top = lax.fori_loop(0, step, first, top)

    diag = jnp.exp(diag - top)
    total = jnp.sum(diag, axis=-1, keepdims=True)

    def second(j, total):
        prob = jnp.exp(score_buf[j] - top)
        score_buf[j] = prob
        return total + jnp.sum(prob, axis=-1, keepdims=True)

    total = lax.fori_loop(0, step, second, total)
    inv = 1.0 / total
    acc = dot_nn((diag * inv).astype(BF16), kv_ref[here, vcol - kcol:])

    def third(j, acc):
        there = pl.ds(pl.multiple_of(j * blk, blk), blk)
        return acc + dot_nn((score_buf[j] * inv).astype(BF16), kv_ref[there, vcol - kcol:])

    acc = lax.fori_loop(0, step, third, acc)
    lse = top + jnp.log(total)
    lane = lax.broadcasted_iota(jnp.int32, (blk, HEAD_DIM), 1)
    packed = jnp.zeros((blk, HEAD_DIM), F32)
    for head in range(heads):
        rws = slice(head * blk, (head + 1) * blk)
        o_out[:, head * HEAD_DIM:(head + 1) * HEAD_DIM] = acc[rws].astype(BF16)
        packed = jnp.where(lane == head, lse[rws], packed)
    lse_out[...] = packed


def attn_forward(qkv, cos_tab, sin_tab, heads, blk=256):
    seq, width = qkv.shape
    hcols = heads * HEAD_DIM
    steps = seq // blk
    row = lambda i: (i, 0)
    flops = 4 * heads * seq * seq * HEAD_DIM // 2
    return pl.pallas_call(
        functools.partial(attn_fwd_body, heads, blk),
        grid=(steps,),
        in_specs=[pl.BlockSpec((blk, width), row), pl.BlockSpec((blk, HEAD_DIM), row), pl.BlockSpec((blk, HEAD_DIM), row), pl.BlockSpec((seq, 2 * HEAD_DIM), lambda i: (0, 0))],
        out_specs=[pl.BlockSpec((blk, hcols), row), pl.BlockSpec((blk, HEAD_DIM), row), pl.BlockSpec((blk, hcols), row), pl.BlockSpec((blk, HEAD_DIM), row)],
        out_shape=[jax.ShapeDtypeStruct((seq, hcols), BF16), jax.ShapeDtypeStruct((seq, HEAD_DIM), BF16), jax.ShapeDtypeStruct((seq, hcols), BF16), jax.ShapeDtypeStruct((seq, HEAD_DIM), F32)],
        scratch_shapes=[pltpu.VMEM((steps, heads * blk, blk), F32), pltpu.VMEM((seq, HEAD_DIM), BF16)],
        compiler_params=pltpu.CompilerParams(dimension_semantics=("arbitrary",), vmem_limit_bytes=40 * 2 ** 20),
        cost_estimate=pl.CostEstimate(flops=flops * 4, bytes_accessed=8 * 2 ** 20, transcendentals=heads * seq * seq // 2),
        name="attn_fwd",
    )(qkv, cos_tab, sin_tab, qkv[:, hcols:])


def attn_bwd_body(heads, blk, q_ref, do_ref, lse_ref, k_ref, v_ref, cos_ref, sin_ref, out_ref, prob_buf, dprob_buf, dk_acc, dv_acc):
    step = pl.program_id(0)
    scale = HEAD_DIM ** -0.5
    rows = heads * blk
    hcols = heads * HEAD_DIM
    here = pl.ds(pl.multiple_of(step * blk, blk), blk)

    @pl.when(step == 0)
    def _():
        dk_acc[...] = jnp.zeros_like(dk_acc)
        dv_acc[...] = jnp.zeros_like(dv_acc)

    def heads_of(ref):
        return jnp.concatenate([ref[:, h * HEAD_DIM:(h + 1) * HEAD_DIM] for h in range(heads)], axis=0)

    query = heads_of(q_ref)
    d_out = heads_of(do_ref)
    lse = jnp.concatenate([lse_ref[:, h:h + 1] for h in range(heads)], axis=0)
    row_id = lax.broadcasted_iota(jnp.int32, (heads, blk, blk), 1).reshape(rows, blk)
    col_id = lax.broadcasted_iota(jnp.int32, (rows, blk), 1)

    def score_part(j, masked):
        there = pl.ds(pl.multiple_of(j * blk, blk), blk)
        score = dot_nt(query, k_ref[there, :]) * scale
        if masked:
            score = jnp.where(row_id >= col_id, score, -1e30)
        prob = jnp.exp(score - lse)
        d_prob = dot_nt(d_out, v_ref[there, :]).astype(BF16)
        prob_buf[j] = prob
        dprob_buf[j] = d_prob
        dv_acc[there, :] += dot_tn(prob.astype(BF16), d_out)
        return jnp.sum(prob * d_prob.astype(F32), axis=-1, keepdims=True)

    row_dot = score_part(step, True)
    row_dot = lax.fori_loop(0, step, lambda j, tot: tot + score_part(j, False), row_dot)

    def grad_part(j, acc):
        there = pl.ds(pl.multiple_of(j * blk, blk), blk)
        d_score = (prob_buf[j] * (dprob_buf[j].astype(F32) - row_dot) * scale).astype(BF16)
        dk_acc[there, :] += dot_tn(d_score, query)
        return acc + dot_nn(d_score, k_ref[there, :])

    d_query = lax.fori_loop(0, step + 1, grad_part, jnp.zeros((rows, HEAD_DIM), F32))
    cos_tab, sin_tab = cos_ref[here, :], sin_ref[here, :]
    for head in range(heads):
        part = d_query[head * blk:(head + 1) * blk].astype(BF16).astype(F32)
        out_ref[here, head * HEAD_DIM:(head + 1) * HEAD_DIM] = turn(part, cos_tab, -sin_tab).astype(BF16)

    @pl.when(step == pl.num_programs(0) - 1)
    def _():
        d_key = dk_acc[...].astype(BF16).astype(F32)
        out_ref[:, hcols:hcols + HEAD_DIM] = turn(d_key, cos_ref[...], -sin_ref[...]).astype(BF16)
        out_ref[:, hcols + HEAD_DIM:] = dv_acc[...].astype(BF16)


def attn_backward(query, d_attn, lse, key, value, cos_tab, sin_tab, heads, blk=256):
    seq = query.shape[0]
    hcols = heads * HEAD_DIM
    width = hcols + 2 * HEAD_DIM
    steps = seq // blk
    row = lambda i: (i, 0)
    whole = lambda i: (0, 0)
    flops = 10 * heads * seq * seq * HEAD_DIM // 2
    return pl.pallas_call(
        functools.partial(attn_bwd_body, heads, blk),
        grid=(steps,),
        in_specs=[pl.BlockSpec((blk, hcols), row), pl.BlockSpec((blk, hcols), row), pl.BlockSpec((blk, HEAD_DIM), row)] + [pl.BlockSpec((seq, HEAD_DIM), whole)] * 4,
        out_specs=pl.BlockSpec((seq, width), whole),
        out_shape=jax.ShapeDtypeStruct((seq, width), BF16),
        scratch_shapes=[pltpu.VMEM((steps, heads * blk, blk), F32), pltpu.VMEM((steps, heads * blk, blk), BF16), pltpu.VMEM((seq, HEAD_DIM), F32), pltpu.VMEM((seq, HEAD_DIM), F32)],
        compiler_params=pltpu.CompilerParams(dimension_semantics=("arbitrary",), vmem_limit_bytes=48 * 2 ** 20),
        cost_estimate=pl.CostEstimate(flops=flops * 4, bytes_accessed=10 * 2 ** 20, transcendentals=heads * seq * seq // 2),
        name="attn_bwd",
    )(query, d_attn, lse, key, value, cos_tab, sin_tab)


def wgrad_body(left_ref, right_ref, *rest):
    out_ref = rest[-1]
    out_ref[0] = dot_tn(left_ref[...], right_ref[...]).astype(BF16)


def weight_grad(left, right, into, layer, n_layers, bm, bn):
    seq, rows = left.shape
    cols = right.shape[1]
    shape = jax.ShapeDtypeStruct((n_layers, rows, cols), BF16)
    in_specs = [pl.BlockSpec((seq, bm), lambda i, j: (0, i)), pl.BlockSpec((seq, bn), lambda i, j: (0, j))]
    operands = [left, right]
    aliases = {}
    if into is not None:
        in_specs.append(pl.BlockSpec(memory_space=pl.ANY))
        operands.append(into)
        aliases = {2: 0}
    return pl.pallas_call(
        wgrad_body,
        grid=(rows // bm, cols // bn),
        in_specs=in_specs,
        out_specs=pl.BlockSpec((1, bm, bn), lambda i, j: (layer, i, j)),
        out_shape=shape,
        input_output_aliases=aliases,
        compiler_params=pltpu.CompilerParams(dimension_semantics=("arbitrary", "arbitrary"), vmem_limit_bytes=48 * 2 ** 20),
        cost_estimate=pl.CostEstimate(flops=2 * seq * rows * cols, bytes_accessed=2 * (seq * (rows + cols) + rows * cols), transcendentals=0),
        name="wgrad",
    )(*operands)


TILE = 256


def rs_body(n_ops, layer, trans, tp_axis, *refs):
    lhs_hbm = refs[:n_ops]
    rhs_hbm = refs[n_ops:2 * n_ops]
    out_ref = refs[2 * n_ops]
    lhs = refs[2 * n_ops + 1:3 * n_ops + 1]
    rhs = refs[3 * n_ops + 1:4 * n_ops + 1]
    (own, stage, pair_in, diag_in, near_in, far_in, last_out, last_in,
     lhs_sem, rhs_sem, pair_ssem, pair_rsem, diag_ssem, diag_rsem, near_ssem, near_rsem, far_ssem, far_rsem, last_ssem, last_rsem) = refs[4 * n_ops + 1:]
    tiles = own.shape[1]
    rblk = own.shape[2]
    half = tiles * TILE
    rows_out = out_ref.shape[0]

    me = lax.axis_index(tp_axis)
    core = lax.rem(me, 2)
    chip = me // 2
    x = lax.rem(chip, 2)
    y = chip // 2
    partner = chip * 2 + (1 - core)
    chip_x = y * 2 + (1 - x)
    chip_y = (1 - y) * 2 + x
    chip_d = (1 - y) * 2 + (1 - x)
    dev_x = chip_x * 2 + core
    dev_y = chip_y * 2 + core
    near = dev_x * (1 - core) + dev_y * core
    far = dev_y * (1 - core) + dev_x * core
    near_slot = 1 + core
    far_slot = 2 - core
    chips = (chip_d, chip_x, chip_y, chip)

    def row_ds(slot):
        return pl.ds(pl.multiple_of(chips[slot] * rblk, rblk), rblk)

    def own_ds(t):
        return pl.ds(pl.multiple_of(core * half + t * TILE, TILE), TILE)

    def pair_ds(t):
        return pl.ds(pl.multiple_of((1 - core) * half + t * TILE, TILE), TILE)

    def lhs_copy(i, slot):
        return pltpu.make_async_copy(lhs_hbm[i].at[row_ds(slot), :], lhs[i].at[row_ds(slot), :], lhs_sem.at[i, slot])

    def rhs_copy(i, cols, which, t):
        if trans:
            return pltpu.make_async_copy(rhs_hbm[i].at[layer, cols, :], rhs[i].at[cols, :], rhs_sem.at[i, which, t])
        return pltpu.make_async_copy(rhs_hbm[i].at[layer, :, cols], rhs[i].at[:, cols], rhs_sem.at[i, which, t])

    for i in range(n_ops):
        lhs_copy(i, 0).start()
    for t in range(tiles):
        for i in range(n_ops):
            rhs_copy(i, pair_ds(t), 0, t).start()
        for i in range(n_ops):
            rhs_copy(i, own_ds(t), 1, t).start()
    for slot in (1, 2, 3):
        for i in range(n_ops):
            lhs_copy(i, slot).start()

    barrier = pltpu.get_barrier_semaphore()
    for other in (partner, dev_x, dev_y):
        pl.semaphore_signal(barrier, inc=1, device_id={tp_axis: other}, device_id_type=pl.DeviceIdType.MESH)
    pl.semaphore_wait(barrier, 3)

    def product(slot, cols):
        acc = None
        for i in range(n_ops):
            left = lhs[i][row_ds(slot), :]
            part = dot_nt(left, rhs[i][cols, :]) if trans else dot_nn(left, rhs[i][:, cols])
            acc = part if acc is None else acc + part
        return acc

    def remote(src, dst, ssem, rsem, target):
        return pltpu.make_async_remote_copy(src_ref=src, dst_ref=dst, send_sem=ssem, recv_sem=rsem, device_id={tp_axis: target}, device_id_type=pl.DeviceIdType.MESH)

    def pair_copy(slot, t):
        spot = t if slot in (0, 2) else tiles + t
        return remote(stage.at[spot], pair_in.at[slot, t], pair_ssem.at[slot, t], pair_rsem.at[slot, t], partner)

    def pair_wait(slot, t):
        remote(stage.at[t], pair_in.at[slot, t], pair_ssem.at[slot, t], pair_rsem.at[slot, t], partner).wait_recv()

    def diag_copy(t):
        return remote(own.at[0, t], diag_in.at[t], diag_ssem.at[t], diag_rsem.at[t], near)

    def near_copy(t):
        return remote(own.at[near_slot, t], near_in.at[t], near_ssem.at[t], near_rsem.at[t], near)

    def far_copy(t):
        return remote(own.at[far_slot, t], far_in.at[t], far_ssem.at[t], far_rsem.at[t], far)

    def last_copy(t):
        return remote(last_out.at[t], last_in.at[t], last_ssem.at[t], last_rsem.at[t], partner)

    def emit_pair(slot, t):
        spot = t if slot in (0, 2) else tiles + t
        stage[spot] = product(slot, pair_ds(t))
        pair_copy(slot, t).start()

    for i in range(n_ops):
        lhs_copy(i, 0).wait()

    def finish_diag(t):
        pair_wait(0, t)
        own[0, t] += pair_in[0, t]
        diag_copy(t).start()

    def diag_step(t, carry):
        for i in range(n_ops):
            rhs_copy(i, pair_ds(t), 0, t).wait()
        emit_pair(0, t)
        for i in range(n_ops):
            rhs_copy(i, own_ds(t), 1, t).wait()
        own[0, t] = product(0, own_ds(t))

        @pl.when(t > 0)
        def _():
            finish_diag(t - 1)
        return carry

    lax.fori_loop(0, tiles, diag_step, 0)
    finish_diag(tiles - 1)

    for slot in (1, 2):
        for i in range(n_ops):
            lhs_copy(i, slot).wait()

    def finish_sides(t):
        pair_wait(near_slot, t)
        own[near_slot, t] += pair_in[near_slot, t]
        near_copy(t).start()
        pair_wait(far_slot, t)
        diag_copy(t).wait_recv()
        own[far_slot, t] += pair_in[far_slot, t] + diag_in[t]
        far_copy(t).start()

    def side_step(t, carry):
        emit_pair(1, t)
        pair_copy(0, t).wait_send()
        emit_pair(2, t)
        own[1, t] = product(1, own_ds(t))
        own[2, t] = product(2, own_ds(t))

        @pl.when(t > 0)
        def _():
            finish_sides(t - 1)
        return carry

    lax.fori_loop(0, tiles, side_step, 0)
    finish_sides(tiles - 1)

    for i in range(n_ops):
        lhs_copy(i, 3).wait()

    def self_step(t, carry):
        pair_copy(1, t).wait_send()
        emit_pair(3, t)
        own[3, t] = product(3, own_ds(t))
        return carry

    lax.fori_loop(0, tiles, self_step, 0)

    def final_step(t, carry):
        pair_wait(3, t)
        near_copy(t).wait_recv()
        own[3, t] += pair_in[3, t] + near_in[t]
        far_copy(t).wait_recv()
        own[3, t] += far_in[t]
        last_out[t] = own[3, t, pl.ds(pl.multiple_of((1 - core) * rows_out, rows_out), rows_out), :]
        last_copy(t).start()
        out_ref[:, own_ds(t)] = own[3, t, pl.ds(pl.multiple_of(core * rows_out, rows_out), rows_out), :]
        return carry

    lax.fori_loop(0, tiles, final_step, 0)

    def close_step(t, carry):
        last_copy(t).wait_recv()
        out_ref[:, pair_ds(t)] = last_in[t]
        pair_copy(2, t).wait_send()
        pair_copy(3, t).wait_send()
        diag_copy(t).wait_send()
        near_copy(t).wait_send()
        far_copy(t).wait_send()
        last_copy(t).wait_send()
        return carry

    lax.fori_loop(0, tiles, close_step, 0)


def matmul_reduce_scatter(lhs_list, rhs_list, layer, trans, tp_axis, tp_size, cid):
    n_ops = len(lhs_list)
    seq = lhs_list[0].shape[0]
    d_model = rhs_list[0].shape[1] if trans else rhs_list[0].shape[2]
    rblk = seq * 2 // tp_size
    tiles = d_model // 2 // TILE
    rows_out = seq // tp_size
    ks = [item.shape[1] for item in lhs_list]
    dma = pltpu.SemaphoreType.DMA
    scratch = [pltpu.VMEM((seq, k), BF16) for k in ks]
    scratch += [pltpu.VMEM((d_model, k) if trans else (k, d_model), BF16) for k in ks]
    scratch += [
        pltpu.VMEM((4, tiles, rblk, TILE), F32),
        pltpu.VMEM((2 * tiles, rblk, TILE), F32),
        pltpu.VMEM((4, tiles, rblk, TILE), F32),
        pltpu.VMEM((tiles, rblk, TILE), F32),
        pltpu.VMEM((tiles, rblk, TILE), F32),
        pltpu.VMEM((tiles, rblk, TILE), F32),
        pltpu.VMEM((tiles, rows_out, TILE), F32),
        pltpu.VMEM((tiles, rows_out, TILE), F32),
        dma((n_ops, 4)), dma((n_ops, 2, tiles)),
        dma((4, tiles)), dma((4, tiles)),
        dma((tiles,)), dma((tiles,)), dma((tiles,)), dma((tiles,)), dma((tiles,)), dma((tiles,)), dma((tiles,)), dma((tiles,)),
    ]
    flops = 2 * seq * d_model * sum(ks)
    return pl.pallas_call(
        functools.partial(rs_body, n_ops, layer, trans, tp_axis),
        in_specs=[pl.BlockSpec(memory_space=pl.ANY)] * (2 * n_ops),
        out_specs=pl.BlockSpec(memory_space=pltpu.VMEM),
        out_shape=jax.ShapeDtypeStruct((rows_out, d_model), F32),
        scratch_shapes=scratch,
        compiler_params=pltpu.CompilerParams(collective_id=cid, has_side_effects=True, vmem_limit_bytes=VMEM_MAX),
        cost_estimate=pl.CostEstimate(flops=flops * 3, bytes_accessed=40 * 2 ** 20, transcendentals=0),
        name="matmul_rs",
    )(*lhs_list, *rhs_list)


def solution(mesh):
    tp_size = mesh.shape['tp']
    row_spec = P(('dp', 'tp'), None)
    col_spec = P(None, None, 'tp')
    inner_spec = P(None, 'tp', None)

    def device_program(x_loc, dy_loc, norm_gain, w_qkv, w_out, w_gate, w_up, w_down):
        n_layers = w_qkv.shape[0]
        heads = w_out.shape[1] // HEAD_DIM
        hcols = heads * HEAD_DIM
        seq = x_loc.shape[0] * tp_size
        cos_tab, sin_tab = rope_tables(seq)
        gather = lambda value: lax.all_gather(value, 'tp', axis=0, tiled=True)
        saved = []
        x_cur = x_loc
        u_full = None
        dy_full = None
        for layer in range(n_layers):
            x_f32 = x_cur.astype(F32)
            u_loc = rms_scale(x_f32, norm_gain[layer]).astype(BF16)
            u_full = gather(u_loc)
            qkv = dot_nn(u_full, w_qkv[layer]).astype(BF16)
            if layer == n_layers - 1:
                qkv, dy_src = lax.optimization_barrier((qkv, dy_loc))
                dy_full = gather(dy_src)
            query, key, attn, lse = attn_forward(qkv, cos_tab, sin_tab, heads)
            gate = dot_nn(u_full, w_gate[layer]).astype(BF16)
            up = dot_nn(u_full, w_up[layer]).astype(BF16)
            saved.append((x_cur, u_loc, query, key, qkv[:, hcols + HEAD_DIM:], attn, lse, gate, up))
            if layer < n_layers - 1:
                hidden = gated(gate.astype(F32), up.astype(F32)).astype(BF16)
                total = matmul_reduce_scatter([attn, hidden], [w_out, w_down], layer, False, 'tp', tp_size, layer)
                x_cur = (x_f32 + total).astype(BF16)

        grads = [None] * 5
        gains = [None] * n_layers
        dy_cur = dy_loc
        for layer in reversed(range(n_layers)):
            x_sav, u_loc, query, key, value, attn, lse, gate, up = saved[layer]
            d_attn = dot_nt(dy_full, w_out[layer]).astype(BF16)
            d_hidden = dot_nt(dy_full, w_down[layer]).astype(BF16)
            hidden_f32, gated_pull = jax.vjp(gated, gate.astype(F32), up.astype(F32))
            hidden = hidden_f32.astype(BF16)
            d_gate_f32, d_up_f32 = gated_pull(d_hidden.astype(F32))
            d_gate = d_gate_f32.astype(BF16)
            d_up = d_up_f32.astype(BF16)
            d_qkv = attn_backward(query, d_attn, lse, key, value, cos_tab, sin_tab, heads)
            total = matmul_reduce_scatter([d_qkv, d_gate, d_up], [w_qkv, w_gate, w_up], layer, True, 'tp', tp_size, n_layers + layer)
            d_normed = total.astype(BF16)
            norm_pull = jax.vjp(rms_scale, x_sav.astype(F32), norm_gain[layer])[1]
            d_x_norm, gains[layer] = norm_pull(d_normed.astype(F32))
            dy_cur = (dy_cur.astype(F32) + d_x_norm).astype(BF16)
            dy_cur, u_full, dy_full, d_qkv, d_gate, d_up, attn, hidden = lax.optimization_barrier((dy_cur, u_full, dy_full, d_qkv, d_gate, d_up, attn, hidden))
            if layer > 0:
                dy_next = gather(dy_cur)
            pairs = [(u_full, d_qkv, 512, d_qkv.shape[1]), (attn, dy_full, hcols, 1024), (u_full, d_gate, 512, d_gate.shape[1]), (u_full, d_up, 512, d_up.shape[1]), (hidden, dy_full, hidden.shape[1], 512)]
            for idx, (left, right, bm, bn) in enumerate(pairs):
                grads[idx] = weight_grad(left, right, grads[idx], layer, n_layers, bm, bn)
            if layer > 0:
                barred = lax.optimization_barrier((dy_next, saved[layer - 1][1], *grads))
                dy_full = barred[0]
                grads = list(barred[2:])
                u_full = gather(barred[1])
        grad_gain = lax.psum(jnp.stack(gains), 'tp')
        return (dy_cur, grad_gain, *grads)

    return jax.shard_map(device_program, mesh=mesh, in_specs=(row_spec, row_spec, P(None, None), col_spec, inner_spec, col_spec, col_spec, inner_spec), out_specs=(row_spec, P('dp', None), P('dp', None, 'tp'), P('dp', 'tp', None), P('dp', None, 'tp'), P('dp', None, 'tp'), P('dp', 'tp', None)), check_vma=False)
```

```python
import functools

import jax
import jax.numpy as jnp
from jax import lax
from jax.experimental import pallas as pl
from jax.experimental.pallas import tpu as pltpu
from jax.sharding import PartitionSpec as P

HEAD_DIM = 128
NORM_EPS = 1e-5
ROPE_BASE = 10000.0
BF16 = jnp.bfloat16
F32 = jnp.float32
VMEM_MAX = 67043328


DIAG, XSIDE, YSIDE, SELF = range(4)
HALVES = range(2)
WHOLE = slice(None)


def loop(count, body):
    def step(i, carry):
        body(i)
        return carry

    lax.fori_loop(0, count, step, 0)


def take(refs, count):
    return [next(refs) for _ in range(count)]


def tile_ds(index, size):
    return pl.ds(pl.multiple_of(index * size, size), size)


def rope_tables(seq_len):
    half_dim = HEAD_DIM // 2
    freqs = ROPE_BASE ** (-2.0 * jnp.arange(half_dim, dtype=F32) / HEAD_DIM)
    angles = jnp.arange(seq_len, dtype=F32)[:, None] * freqs[None, :]
    cos, sin = jnp.cos(angles), jnp.sin(angles)
    return jnp.concatenate([cos, cos], axis=1), jnp.concatenate([-sin, sin], axis=1)


def rms_scale(x_f32, gain_row):
    inv_rms = lax.rsqrt(jnp.mean(x_f32 * x_f32, axis=-1, keepdims=True) + NORM_EPS)
    return x_f32 * inv_rms * gain_row


def gated(gate_f32, up_f32):
    return jax.nn.silu(gate_f32) * up_f32


def dot_nt(lhs, rhs):
    return lax.dot_general(lhs, rhs, (((1,), (1,)), ((), ())), preferred_element_type=F32)


def dot_tn(lhs, rhs):
    return lax.dot_general(lhs, rhs, (((0,), (0,)), ((), ())), preferred_element_type=F32)


def dot_nn(lhs, rhs):
    return lax.dot_general(lhs, rhs, (((1,), (0,)), ((), ())), preferred_element_type=F32)


def turn(values, cos_tab, sin_tab):
    return values * cos_tab + pltpu.roll(values, HEAD_DIM // 2, 1) * sin_tab


def ring_ids(tp_axis):
    me = lax.axis_index(tp_axis)
    core = lax.rem(me, 2)
    chip = me // 2
    x = lax.rem(chip, 2)
    y = chip // 2
    chips = ((1 - y) * 2 + (1 - x), y * 2 + (1 - x), (1 - y) * 2 + x, chip)
    partner = chip * 2 + (1 - core)
    dev_x = chips[1] * 2 + core
    dev_y = chips[2] * 2 + core
    near = dev_x * (1 - core) + dev_y * core
    far = dev_y * (1 - core) + dev_x * core
    return core, chips, partner, dev_x, dev_y, near, far


def greet(tp_axis, others):
    barrier = pltpu.get_barrier_semaphore()
    for other in others:
        pl.semaphore_signal(barrier, device_id={tp_axis: other}, device_id_type=pl.DeviceIdType.MESH)
    pl.semaphore_wait(barrier, len(others))


def remote_copy(tp_axis, src, dst, ssem, rsem, target):
    return pltpu.make_async_remote_copy(src_ref=src, dst_ref=dst, send_sem=ssem, recv_sem=rsem, device_id={tp_axis: target}, device_id_type=pl.DeviceIdType.MESH)


class PushGather:
    def __init__(self, tp_axis, src, dst, sems):
        self.tp_axis, self.src, self.dst = tp_axis, src, dst
        self.near_sem, self.far_sem, self.fwd_sem, self.ici_sem, self.pair_ssem, self.pair_rsem, self.own_sem = sems
        self.core, self.chips, self.partner, self.dev_x, self.dev_y, self.near, self.far = ring_ids(tp_axis)
        self.rows = src.shape[0]
        near_chip = self.chips[1] * (1 - self.core) + self.chips[2] * self.core
        far_chip = self.chips[2] * (1 - self.core) + self.chips[1] * self.core
        self.order = (self.chips[3], near_chip, far_chip, self.chips[0])

    def spot(self, chip, core):
        return self.dst.at[pl.ds(pl.multiple_of((chip * 2 + core) * self.rows, self.rows), self.rows), :]

    def remote(self, src, dst, ssem, rsem, target):
        return remote_copy(self.tp_axis, src, dst, ssem, rsem, target)

    def mine(self):
        return self.spot(self.chips[3], self.core)

    def near_copy(self):
        return self.remote(self.src, self.mine(), self.near_sem, self.ici_sem.at[1], self.near)

    def far_copy(self):
        return self.remote(self.src, self.mine(), self.far_sem, self.ici_sem.at[2], self.far)

    def fwd_copy(self):
        block = self.spot(self.order[1], self.core)
        return self.remote(block, block, self.fwd_sem, self.ici_sem.at[3], self.far)

    def pair_copy(self, k):
        block = self.spot(self.order[k], self.core)
        return self.remote(self.src if k == 0 else block, block, self.pair_ssem.at[k], self.pair_rsem.at[self.slot(k)], self.partner)

    def slot(self, k):
        return (0, 2, 1, 3)[k]

    def own_copy(self):
        return pltpu.make_async_copy(self.src, self.mine(), self.own_sem)

    def start(self):
        greet(self.tp_axis, (self.partner, self.dev_x, self.dev_y))
        self.near_copy().start()
        self.far_copy().start()
        self.pair_copy(0).start()
        self.own_copy().start()

    def ici_arrived(self, k):
        block = self.spot(self.order[k], self.core)
        self.remote(self.src, block, self.near_sem, self.ici_sem.at[k], self.near).wait_recv()

    def pass_sides(self):
        self.ici_arrived(1)
        self.fwd_copy().start()
        self.pair_copy(1).start()
        self.ici_arrived(2)
        self.pair_copy(2).start()

    def finish(self):
        self.ici_arrived(3)
        self.pair_copy(3).start()
        self.own_copy().wait()
        self.near_copy().wait_send()
        self.far_copy().wait_send()
        self.fwd_copy().wait_send()
        for k in range(4):
            self.pair_copy(k).wait_send()
            block = self.spot(self.order[k], 1 - self.core)
            self.remote(self.src, block, self.pair_ssem.at[k], self.pair_rsem.at[k], self.partner).wait_recv()


def push_sems():
    dma = pltpu.SemaphoreType.DMA
    return [dma(()), dma(()), dma(()), dma((4,)), dma((4,)), dma((4,)), dma(())]


def fold(values, op):
    acc = values[:, :HEAD_DIM]
    for at in range(HEAD_DIM, values.shape[1], HEAD_DIM):
        acc = op(acc, values[:, at:at + HEAD_DIM])
    return acc


def attn_fwd_body(heads, blk, tp_axis, part, qkv_ref, cos_ref, sin_ref, v_ref, dy_hbm, q_out, k_out, v_out, o_out, lse_out, dy_full, score_buf, k_rot, *sems):
    step = pl.program_id(0)
    width = dy_full.shape[1]
    push = PushGather(tp_axis, dy_hbm.at[:, pl.ds(part * width, width)], dy_full, sems)

    @pl.when(step == 0)
    def _():
        push.start()

    @pl.when(step == pl.num_programs(0) - 1)
    def _():
        push.pass_sides()
    scale = HEAD_DIM ** -0.5
    kcol = heads * HEAD_DIM
    vcol = kcol + HEAD_DIM
    cos_tab, sin_tab = cos_ref[...], sin_ref[...]
    here = tile_ds(step, blk)
    key = turn(qkv_ref[:, kcol:vcol].astype(F32), cos_tab, sin_tab).astype(BF16)
    k_rot[here, :] = key
    k_out[...] = key
    v_out[...] = qkv_ref[:, vcol:]
    parts = []
    for head in range(heads):
        cols = slice(head * HEAD_DIM, (head + 1) * HEAD_DIM)
        part = turn(qkv_ref[:, cols].astype(F32), cos_tab, sin_tab).astype(BF16)
        q_out[:, cols] = part
        parts.append(part)
    query = jnp.concatenate(parts, axis=0)
    rows = heads * blk

    diag = dot_nt(query, key) * scale
    row_id = lax.broadcasted_iota(jnp.int32, (heads, blk, blk), 1).reshape(rows, blk)
    col_id = lax.broadcasted_iota(jnp.int32, (rows, blk), 1)
    diag = jnp.where(row_id >= col_id, diag, -1e30)
    top = fold(diag, jnp.maximum)

    def first(j, top):
        there = tile_ds(j, blk)
        score = dot_nt(query, k_rot[there, :]) * scale
        score_buf[j] = score
        return jnp.maximum(top, fold(score, jnp.maximum))

    top = jnp.max(lax.fori_loop(0, step, first, top), axis=-1, keepdims=True)

    diag = jnp.exp(diag - top)
    total = fold(diag, jnp.add)

    def second(j, total):
        prob = jnp.exp(score_buf[j] - top)
        score_buf[j] = prob
        return total + fold(prob, jnp.add)

    total = jnp.sum(lax.fori_loop(0, step, second, total), axis=-1, keepdims=True)
    inv = 1.0 / total
    acc = dot_nn((diag * inv).astype(BF16), v_ref[here, :])

    def third(j, acc):
        there = tile_ds(j, blk)
        return acc + dot_nn((score_buf[j] * inv).astype(BF16), v_ref[there, :])

    acc = lax.fori_loop(0, step, third, acc)
    lse = top + jnp.log(total)
    lane = lax.broadcasted_iota(jnp.int32, (blk, HEAD_DIM), 1)
    packed = jnp.zeros((blk, HEAD_DIM), F32)
    for head in range(heads):
        rws = slice(head * blk, (head + 1) * blk)
        o_out[:, head * HEAD_DIM:(head + 1) * HEAD_DIM] = acc[rws].astype(BF16)
        packed = jnp.where(lane == head, lse[rws], packed)
    lse_out[...] = packed

    @pl.when(step == pl.num_programs(0) - 1)
    def _():
        push.finish()


def attn_forward(qkv, cos_tab, sin_tab, dy_loc, heads, tp_axis, cid, part, n_parts, blk=384):
    seq, width = qkv.shape
    hcols = heads * HEAD_DIM
    steps = seq // blk
    row = lambda i: (i, 0)
    flops = 4 * heads * seq * seq * HEAD_DIM // 2
    return pl.pallas_call(
        functools.partial(attn_fwd_body, heads, blk, tp_axis, part),
        grid=(steps,),
        in_specs=[pl.BlockSpec((blk, width), row), pl.BlockSpec((blk, HEAD_DIM), row), pl.BlockSpec((blk, HEAD_DIM), row), pl.BlockSpec((seq, HEAD_DIM), lambda i: (0, heads + 1)), pl.BlockSpec(memory_space=pl.ANY)],
        out_specs=[pl.BlockSpec((blk, hcols), row), pl.BlockSpec((blk, HEAD_DIM), row), pl.BlockSpec((blk, HEAD_DIM), row), pl.BlockSpec((blk, hcols), row), pl.BlockSpec((blk, HEAD_DIM), row), pl.BlockSpec(memory_space=pl.ANY)],
        out_shape=[jax.ShapeDtypeStruct((seq, hcols), BF16), jax.ShapeDtypeStruct((seq, HEAD_DIM), BF16), jax.ShapeDtypeStruct((seq, HEAD_DIM), BF16), jax.ShapeDtypeStruct((seq, hcols), BF16), jax.ShapeDtypeStruct((seq, HEAD_DIM), F32), jax.ShapeDtypeStruct((seq, dy_loc.shape[1] // n_parts), BF16)],
        scratch_shapes=[pltpu.VMEM((steps, heads * blk, blk), F32), pltpu.VMEM((seq, HEAD_DIM), BF16)] + push_sems(),
        compiler_params=pltpu.CompilerParams(collective_id=cid, has_side_effects=True, dimension_semantics=("arbitrary",), vmem_limit_bytes=VMEM_MAX),
        cost_estimate=pl.CostEstimate(flops=flops * 4, bytes_accessed=8 * 2 ** 20, transcendentals=heads * seq * seq // 2),
        name="attn_fwd",
    )(qkv, cos_tab, sin_tab, qkv, dy_loc)


def attn_bwd_body(heads, blk, q_ref, do_ref, lse_ref, k_ref, v_ref, cos_ref, sin_ref, out_ref, prob_buf, dprob_buf, dk_acc, dv_acc):
    step = pl.program_id(0)
    scale = HEAD_DIM ** -0.5
    rows = heads * blk
    hcols = heads * HEAD_DIM
    here = tile_ds(step, blk)

    @pl.when(step == 0)
    def _():
        dk_acc[...] = jnp.zeros_like(dk_acc)
        dv_acc[...] = jnp.zeros_like(dv_acc)

    def heads_of(ref):
        return jnp.concatenate([ref[:, h * HEAD_DIM:(h + 1) * HEAD_DIM] for h in range(heads)], axis=0)

    query = heads_of(q_ref)
    d_out = heads_of(do_ref)
    lse = jnp.concatenate([lse_ref[:, h:h + 1] for h in range(heads)], axis=0)
    row_id = lax.broadcasted_iota(jnp.int32, (heads, blk, blk), 1).reshape(rows, blk)
    col_id = lax.broadcasted_iota(jnp.int32, (rows, blk), 1)

    def score_part(j, masked):
        there = tile_ds(j, blk)
        score = dot_nt(query, k_ref[there, :]) * scale
        if masked:
            score = jnp.where(row_id >= col_id, score, -1e30)
        prob = jnp.exp(score - lse)
        d_prob = dot_nt(d_out, v_ref[there, :]).astype(BF16)
        prob_buf[j] = prob
        dprob_buf[j] = d_prob
        dv_acc[there, :] += dot_tn(prob.astype(BF16), d_out)
        return fold(prob * d_prob.astype(F32), jnp.add)

    row_dot = score_part(step, True)
    row_dot = lax.fori_loop(0, step, lambda j, tot: tot + score_part(j, False), row_dot)
    row_dot = jnp.sum(row_dot, axis=-1, keepdims=True)

    def grad_part(j, acc):
        there = tile_ds(j, blk)
        d_score = (prob_buf[j] * (dprob_buf[j].astype(F32) - row_dot) * scale).astype(BF16)
        dk_acc[there, :] += dot_tn(d_score, query)
        return acc + dot_nn(d_score, k_ref[there, :])

    d_query = lax.fori_loop(0, step + 1, grad_part, jnp.zeros((rows, HEAD_DIM), F32))
    cos_tab, sin_tab = cos_ref[here, :], sin_ref[here, :]
    for head in range(heads):
        part = d_query[head * blk:(head + 1) * blk].astype(BF16).astype(F32)
        out_ref[here, head * HEAD_DIM:(head + 1) * HEAD_DIM] = turn(part, cos_tab, -sin_tab).astype(BF16)

    @pl.when(step == pl.num_programs(0) - 1)
    def _():
        d_key = dk_acc[...].astype(BF16).astype(F32)
        out_ref[:, hcols:hcols + HEAD_DIM] = turn(d_key, cos_ref[...], -sin_ref[...]).astype(BF16)
        out_ref[:, hcols + HEAD_DIM:] = dv_acc[...].astype(BF16)


def attn_backward(query, d_attn, lse, key, value, cos_tab, sin_tab, heads, blk=384):
    seq = query.shape[0]
    hcols = heads * HEAD_DIM
    width = hcols + 2 * HEAD_DIM
    steps = seq // blk
    row = lambda i: (i, 0)
    whole = lambda i: (0, 0)
    flops = 10 * heads * seq * seq * HEAD_DIM // 2
    return pl.pallas_call(
        functools.partial(attn_bwd_body, heads, blk),
        grid=(steps,),
        in_specs=[pl.BlockSpec((blk, hcols), row), pl.BlockSpec((blk, hcols), row), pl.BlockSpec((blk, HEAD_DIM), row)] + [pl.BlockSpec((seq, HEAD_DIM), whole)] * 4,
        out_specs=pl.BlockSpec((seq, width), whole),
        out_shape=jax.ShapeDtypeStruct((seq, width), BF16),
        scratch_shapes=[pltpu.VMEM((steps, heads * blk, blk), F32), pltpu.VMEM((steps, heads * blk, blk), BF16), pltpu.VMEM((seq, HEAD_DIM), F32), pltpu.VMEM((seq, HEAD_DIM), F32)],
        compiler_params=pltpu.CompilerParams(dimension_semantics=("arbitrary",), vmem_limit_bytes=VMEM_MAX),
        cost_estimate=pl.CostEstimate(flops=flops * 4, bytes_accessed=10 * 2 ** 20, transcendentals=heads * seq * seq // 2),
        name="attn_bwd",
    )(query, d_attn, lse, key, value, cos_tab, sin_tab)


def dgrad_body(n_parts, *refs):
    parts = refs[:n_parts]
    wo_ref, wd_ref, gate_ref, up_ref, dattn_ref, dgate_ref, dup_ref, hid_ref = refs[n_parts:]

    def product(w_ref, rows):
        acc, at = None, 0
        for part in parts:
            width = part.shape[1]
            term = dot_nt(part[...], w_ref[0, rows, at:at + width])
            acc = term if acc is None else acc + term
            at += width
        return acc.astype(BF16)

    dattn_ref[...] = product(wo_ref, slice(None))
    for t in range(gate_ref.shape[1] // WIDE):
        cols = slice(t * WIDE, (t + 1) * WIDE)
        d_hidden = product(wd_ref, cols)
        hidden, pull = jax.vjp(gated, gate_ref[:, cols].astype(F32), up_ref[:, cols].astype(F32))
        d_gate, d_up = pull(d_hidden.astype(F32))
        hid_ref[:, cols] = hidden.astype(BF16)
        dgate_ref[:, cols] = d_gate.astype(BF16)
        dup_ref[:, cols] = d_up.astype(BF16)


def cotangents(dy_parts, w_out, w_down, gate, up, layer, blk=512):
    seq, fcols = gate.shape
    hcols, d_model = w_out.shape[1:]
    row = lambda i: (i, 0)
    flops = 2 * seq * d_model * (hcols + fcols)
    wide = pl.BlockSpec((blk, fcols), row)
    return pl.pallas_call(
        functools.partial(dgrad_body, len(dy_parts)),
        grid=(seq // blk,),
        in_specs=[pl.BlockSpec((blk, part.shape[1]), row) for part in dy_parts] + [pl.BlockSpec((1, hcols, d_model), lambda i: (layer, 0, 0)), pl.BlockSpec((1, fcols, d_model), lambda i: (layer, 0, 0)), wide, wide],
        out_specs=[pl.BlockSpec((blk, hcols), row), wide, wide, wide],
        out_shape=[jax.ShapeDtypeStruct((seq, hcols), BF16)] + [jax.ShapeDtypeStruct((seq, fcols), BF16)] * 3,
        compiler_params=pltpu.CompilerParams(dimension_semantics=("arbitrary",), vmem_limit_bytes=VMEM_MAX),
        cost_estimate=pl.CostEstimate(flops=flops, bytes_accessed=32 * 2 ** 20, transcendentals=seq * fcols),
        name="cotangents",
    )(*dy_parts, w_out, w_down, gate, up)


def tail_body(n_parts, each, *refs):
    attn_ref, hid_ref = refs[:2]
    parts = refs[2:2 + n_parts]
    q_ref, g_ref, u_ref = refs[2 + n_parts:5 + n_parts]
    q_out, out_out, g_out, u_out, down_out = refs[-5:]
    step = pl.program_id(0)
    for n, part in enumerate(parts):
        @pl.when(step // each == n)
        def _():
            right = part[...]
            out_out[0] = dot_tn(attn_ref[...], right).astype(BF16)
            down_out[0] = dot_tn(hid_ref[...], right).astype(BF16)
    q_out[0] = q_ref[...]
    g_out[0] = g_ref[...]
    u_out[0] = u_ref[...]


def tail_grads(attn, hidden, dy_parts, ready, grads, layer, n_layers, blk=512):
    seq = attn.shape[0]
    width = dy_parts[0].shape[1]
    d_model = width * len(dy_parts)
    each = width // blk
    whole = lambda j: (0, 0)
    hbm = pl.BlockSpec(memory_space=pl.ANY)
    rows = lambda width: pl.BlockSpec((blk, width), lambda j: (j, 0))
    rows_out = lambda width: pl.BlockSpec((1, blk, width), lambda j: (layer, j, 0))
    cols_out = lambda height: pl.BlockSpec((1, height, blk), lambda j: (layer, 0, j))
    part_spec = lambda n: pl.BlockSpec((seq, blk), lambda j: (0, jnp.clip(j - n * each, 0, each - 1)))
    hcols, fcols = attn.shape[1], hidden.shape[1]
    widths = [item.shape[1] for item in ready]
    old = [item for item in grads if item is not None]
    before = 5 + len(dy_parts)
    return pl.pallas_call(
        functools.partial(tail_body, len(dy_parts), each),
        grid=(d_model // blk,),
        in_specs=[pl.BlockSpec((seq, hcols), whole), pl.BlockSpec((seq, fcols), whole)] + [part_spec(n) for n in range(len(dy_parts))] + [rows(w) for w in widths] + [hbm] * len(old),
        out_specs=[rows_out(widths[0]), cols_out(hcols), rows_out(widths[1]), rows_out(widths[2]), cols_out(fcols)],
        out_shape=[jax.ShapeDtypeStruct((n_layers,) + dims, BF16) for dims in ((d_model, widths[0]), (hcols, d_model), (d_model, widths[1]), (d_model, widths[2]), (fcols, d_model))],
        input_output_aliases={before + n: n for n in range(len(old))},
        compiler_params=pltpu.CompilerParams(dimension_semantics=("arbitrary",), vmem_limit_bytes=VMEM_MAX),
        cost_estimate=pl.CostEstimate(flops=2 * seq * d_model * (hcols + fcols), bytes_accessed=60 * 2 ** 20, transcendentals=0),
        name="tail_grads",
    )(attn, hidden, *dy_parts, *ready, *old)


TILE = 256
WIDE = 512
NORM_ROWS = 16


def fill_weight_grads(u_hbm, grads, lhs, rhs, sems):
    load_sem, store_sem = sems
    seq, d_model = u_hbm.shape
    steps = d_model // TILE

    def cols_of(slot):
        return tile_ds(slot, TILE)

    def load(j, slot):
        return pltpu.make_async_copy(u_hbm.at[:, cols_of(j)], rhs[2].at[0:seq, cols_of(slot)], load_sem.at[slot])

    def rows_at(base, slot):
        return pl.ds(pl.multiple_of(base + slot * TILE, TILE), TILE)

    def spots(slot):
        return rhs[0].at[rows_at(seq, slot), :], rhs[1].at[rows_at(seq, slot), :], rhs[1].at[rows_at(seq + 2 * TILE, slot), :]

    def stores(j, slot):
        return [pltpu.make_async_copy(src, dst.at[cols_of(j), :], store_sem.at[slot, n]) for n, (src, dst) in enumerate(zip(spots(slot), grads))]

    load(0, 0).start()

    def step(j):
        slot = lax.rem(j, 2)
        load(j, slot).wait()

        @pl.when(j + 1 < steps)
        def _():
            load(j + 1, 1 - slot).start()

        @pl.when(j >= 2)
        def _():
            for copy in stores(j - 2, slot):
                copy.wait()
        left = rhs[2][0:seq, cols_of(slot)]
        for spot, right in zip(spots(slot), lhs):
            spot[...] = dot_tn(left, right[...]).astype(BF16)
        for copy in stores(j, slot):
            copy.start()

    loop(steps, step)
    for j in (steps - 2, steps - 1):
        for copy in stores(j, j % 2):
            copy.wait()


def rs_body(n_ops, layer, trans, back, tp_axis, *refs):
    refs = iter(refs)
    lhs_hbm = take(refs, n_ops)
    rhs_hbm = take(refs, n_ops)
    if back:
        u_hbm, x_ref, gain_ref, dy_ref, dy_out, gain_out = take(refs, 6)
        grad_hbm = take(refs, n_ops)
    out_ref = next(refs)
    lhs = take(refs, n_ops)
    rhs = take(refs, n_ops)
    (own, stage, pair_in, diag_in, near_in, far_in, last_out, last_in,
     lhs_sem, rhs_sem, pair_ssem, pair_rsem, diag_ssem, diag_rsem, near_ssem, near_rsem, far_ssem, far_rsem, last_ssem, last_rsem) = take(refs, 20)
    fill_sems = list(refs)
    tiles, rblk = own.shape[1:3]
    rows_out = rblk // 2
    core, chips, partner, dev_x, dev_y, near, far = ring_ids(tp_axis)
    other = 1 - core
    near_slot = XSIDE + core
    far_slot = YSIDE - core

    def row_ds(slot):
        return tile_ds(chips[slot], rblk)

    def own_ds(t):
        return tile_ds(core * tiles + t, TILE)

    def pair_ds(t):
        return tile_ds(other * tiles + t, TILE)

    def lhs_copy(i, slot):
        return pltpu.make_async_copy(lhs_hbm[i].at[row_ds(slot), :], lhs[i].at[row_ds(slot), :], lhs_sem.at[i, slot])

    def rhs_copy(i, cols, which, t):
        if trans:
            return pltpu.make_async_copy(rhs_hbm[i].at[layer, cols, :], rhs[i].at[cols, :], rhs_sem.at[i, which, t])
        return pltpu.make_async_copy(rhs_hbm[i].at[layer, :, cols], rhs[i].at[:, cols], rhs_sem.at[i, which, t])

    def pair_load(i, t):
        return rhs_copy(i, pair_ds(t), 0, t)

    def own_load(i, t):
        return rhs_copy(i, own_ds(t), 1, t)

    ops = range(n_ops)
    for i in ops:
        lhs_copy(i, DIAG).start()
    for t in range(tiles):
        for i in ops:
            pair_load(i, t).start()
        for i in ops:
            own_load(i, t).start()
    for slot in (XSIDE, YSIDE, SELF):
        for i in ops:
            lhs_copy(i, slot).start()

    greet(tp_axis, (partner, dev_x, dev_y))

    def product(slot, cols):
        acc = None
        for i in range(n_ops):
            left = lhs[i][row_ds(slot), :]
            part = dot_nt(left, rhs[i][cols, :]) if trans else dot_nn(left, rhs[i][:, cols])
            acc = part if acc is None else acc + part
        return acc

    remote = functools.partial(remote_copy, tp_axis)

    def spot(slot, t):
        return stage.at[t if slot in (DIAG, YSIDE) else tiles + t]

    def pair_copy(slot, t):
        return remote(spot(slot, t), pair_in.at[slot, t], pair_ssem.at[slot, t], pair_rsem.at[slot, t], partner)

    def pair_wait(slot, t):
        remote(stage.at[t], pair_in.at[slot, t], pair_ssem.at[slot, t], pair_rsem.at[slot, t], partner).wait_recv()

    def diag_copy(t):
        return remote(own.at[DIAG, t], diag_in.at[t], diag_ssem.at[t], diag_rsem.at[t], near)

    def near_copy(t):
        return remote(own.at[near_slot, t], near_in.at[t], near_ssem.at[t], near_rsem.at[t], near)

    def far_copy(t):
        return remote(own.at[far_slot, t], far_in.at[t], far_ssem.at[t], far_rsem.at[t], far)

    def last_copy(t):
        return remote(last_out.at[t], last_in.at[t], last_ssem.at[t], last_rsem.at[t], partner)

    def emit_pair(slot, t):
        spot(slot, t)[...] = product(slot, pair_ds(t))
        pair_copy(slot, t).start()

    for i in ops:
        lhs_copy(i, DIAG).wait()

    def finish_diag(t):
        pair_wait(DIAG, t)
        own[DIAG, t] += pair_in[DIAG, t]
        diag_copy(t).start()

    def lagged(finish, t):
        @pl.when(t == 0)
        def _():
            finish(t)

        @pl.when(t > 1)
        def _():
            finish(t - 1)

    def diag_step(t):
        for i in ops:
            pair_load(i, t).wait()
        emit_pair(DIAG, t)
        for i in ops:
            own_load(i, t).wait()
        own[DIAG, t] = product(DIAG, own_ds(t))
        lagged(finish_diag, t)

    loop(tiles, diag_step)
    finish_diag(tiles - 1)

    for slot in (XSIDE, YSIDE):
        for i in ops:
            lhs_copy(i, slot).wait()

    def finish_sides(t):
        pair_wait(near_slot, t)
        own[near_slot, t] += pair_in[near_slot, t]
        near_copy(t).start()
        pair_wait(far_slot, t)
        diag_copy(t).wait_recv()
        own[far_slot, t] += pair_in[far_slot, t] + diag_in[t]
        far_copy(t).start()

    def side_step(t):
        emit_pair(XSIDE, t)
        pair_copy(DIAG, t).wait_send()
        emit_pair(YSIDE, t)
        own[XSIDE, t] = product(XSIDE, own_ds(t))
        own[YSIDE, t] = product(YSIDE, own_ds(t))
        lagged(finish_sides, t)

    loop(tiles, side_step)
    finish_sides(tiles - 1)

    for i in ops:
        lhs_copy(i, SELF).wait()

    def self_step(t):
        pair_copy(XSIDE, t).wait_send()
        emit_pair(SELF, t)
        own[SELF, t] = product(SELF, own_ds(t))

    loop(tiles, self_step)

    if back:
        fill_weight_grads(u_hbm, grad_hbm, lhs, rhs, fill_sems)

    def final_step(t):
        pair_wait(SELF, t)
        near_copy(t).wait_recv()
        own[SELF, t] += pair_in[SELF, t] + near_in[t]
        far_copy(t).wait_recv()
        own[SELF, t] += far_in[t]
        last_out[t] = own[SELF, t, tile_ds(other, rows_out), :]
        last_copy(t).start()
        out_ref[:, own_ds(t)] = own[SELF, t, tile_ds(core, rows_out), :]

    loop(tiles, final_step)

    def close_step(t):
        last_copy(t).wait_recv()
        out_ref[:, pair_ds(t)] = last_in[t]
        for copy in (pair_copy(YSIDE, t), pair_copy(SELF, t), diag_copy(t), near_copy(t), far_copy(t), last_copy(t)):
            copy.wait_send()

    loop(tiles, close_step)

    if back:
        gain = gain_ref[...]
        gain_out[...] = jnp.zeros_like(gain)

        def norm_step(r):
            rows = tile_ds(r, NORM_ROWS)
            pull = jax.vjp(rms_scale, x_ref[rows, :].astype(F32), gain)[1]
            d_x, d_gain = pull(out_ref[rows, :].astype(BF16).astype(F32))
            dy_out[rows, :] = (dy_ref[rows, :].astype(F32) + d_x).astype(BF16)
            gain_out[...] += d_gain

        loop(rows_out // NORM_ROWS, norm_step)


def matmul_reduce_scatter(lhs_list, rhs_list, layer, trans, tp_axis, tp_size, cid, norm=None):
    n_ops = len(lhs_list)
    seq = lhs_list[0].shape[0]
    d_model = rhs_list[0].shape[1] if trans else rhs_list[0].shape[2]
    rblk = seq * 2 // tp_size
    tiles = d_model // 2 // TILE
    rows_out = seq // tp_size
    ks = [item.shape[1] for item in lhs_list]
    dma = pltpu.SemaphoreType.DMA
    scratch = [pltpu.VMEM((seq, k), BF16) for k in ks]
    scratch += [pltpu.VMEM((d_model, k) if trans else (k, d_model), BF16) for k in ks]
    scratch += [
        pltpu.VMEM((4, tiles, rblk, TILE), F32),
        pltpu.VMEM((2 * tiles, rblk, TILE), F32),
        pltpu.VMEM((4, tiles, rblk, TILE), F32),
        pltpu.VMEM((tiles, rblk, TILE), F32),
        pltpu.VMEM((tiles, rblk, TILE), F32),
        pltpu.VMEM((tiles, rblk, TILE), F32),
        pltpu.VMEM((tiles, rows_out, TILE), F32),
        pltpu.VMEM((tiles, rows_out, TILE), F32),
        dma((n_ops, 4)), dma((n_ops, 2, tiles)),
        dma((4, tiles)), dma((4, tiles)),
    ] + [dma((tiles,))] * 8
    flops = 2 * seq * d_model * sum(ks)
    hbm = pl.BlockSpec(memory_space=pl.ANY)
    vmem = pl.BlockSpec(memory_space=pltpu.VMEM)
    operands = list(lhs_list) + list(rhs_list)
    in_specs = [hbm] * len(operands)
    out_specs, out_shape = [vmem], [jax.ShapeDtypeStruct((rows_out, d_model), F32)]
    if norm is not None:
        operands += norm
        in_specs += [hbm] + [vmem] * (len(norm) - 1)
        scratch = [pltpu.VMEM((rows_out, d_model), F32)] + scratch + [dma((2,)), dma((2, 3))]
        out_specs = [vmem] * 2 + [hbm] * n_ops
        out_shape = [jax.ShapeDtypeStruct((rows_out, d_model), BF16), jax.ShapeDtypeStruct((1, d_model), F32)]
        out_shape += [jax.ShapeDtypeStruct((d_model, k), BF16) for k in ks]
    return pl.pallas_call(
        functools.partial(rs_body, n_ops, layer, trans, norm is not None, tp_axis),
        in_specs=in_specs,
        out_specs=out_specs,
        out_shape=out_shape,
        scratch_shapes=scratch,
        compiler_params=pltpu.CompilerParams(collective_id=cid, has_side_effects=True, vmem_limit_bytes=VMEM_MAX),
        cost_estimate=pl.CostEstimate(flops=flops * 3, bytes_accessed=40 * 2 ** 20, transcendentals=0),
        name="matmul_rs",
    )(*operands)


def ag_body(layer, with_total, with_hidden, with_u, tp_axis, *refs):
    refs = iter(refs)
    n_stage = 3 + with_hidden
    n_res = n_stage + with_u
    x_ref = next(refs)
    if with_total:
        total_ref = next(refs)
    gain_ref, wq_hbm, wg_hbm, wu_hbm = take(refs, 4)
    if with_total:
        x_out = next(refs)
    u_out = next(refs)
    res_hbm = take(refs, n_res)
    wq, wg, wu, ubuf = take(refs, 4)
    stage = take(refs, n_stage)
    w_sem, x_ssem, y_ssem, ici_rsem, fwd_ssem, pair_ssem, pair_rsem, out_sem = refs
    piece = ubuf.shape[1]

    core, chips, partner, dev_x, dev_y, near, far = ring_ids(tp_axis)
    qcols = wq.shape[1]
    fcols = wg.shape[1]
    qtiles = [(s, min(WIDE, qcols - s)) for s in range(0, qcols, WIDE)]
    ftiles = fcols // WIDE

    def w_copy(k):
        if k < len(qtiles):
            cols = slice(qtiles[k][0], qtiles[k][0] + qtiles[k][1])
            return pltpu.make_async_copy(wq_hbm.at[layer, :, cols], wq.at[:, cols], w_sem.at[k])
        t, which = divmod(k - len(qtiles), 2)
        cols = slice(t * WIDE, (t + 1) * WIDE)
        src, dst = ((wg_hbm, wg), (wu_hbm, wu))[which]
        return pltpu.make_async_copy(src.at[layer, :, cols], dst.at[:, cols], w_sem.at[k])

    n_w = len(qtiles) + 2 * ftiles
    for k in range(n_w):
        w_copy(k).start()

    def spot(group, cc):
        return group * 2 + cc

    gain = gain_ref[...]
    for half in HALVES:
        rows = tile_ds(half, piece)
        x_f32 = x_ref[rows, :].astype(F32)
        if with_total:
            x_new = (x_f32 + total_ref[rows, :]).astype(BF16)
            x_out[rows, :] = x_new
            x_f32 = x_new.astype(F32)
        u_new = rms_scale(x_f32, gain).astype(BF16)
        u_out[rows, :] = u_new
        ubuf[spot(half, core)] = u_new
    greet(tp_axis, (partner, dev_x, dev_y))

    remote = functools.partial(remote_copy, tp_axis)

    def x_group(half):
        return 2 + 2 * half

    def y_group(half):
        return 3 + 2 * half

    def d_group(half):
        return 6 + half

    def my_piece(group):
        return ubuf.at[spot(group, core)]

    def x_copy(half):
        return remote(my_piece(half), my_piece(x_group(half)), x_ssem.at[half], ici_rsem.at[x_group(half)], dev_x)

    def y_copy(half):
        return remote(my_piece(half), my_piece(y_group(half)), y_ssem.at[half], ici_rsem.at[y_group(half)], dev_y)

    def fwd_copy(half):
        return remote(my_piece(x_group(half) + core), my_piece(d_group(half)), fwd_ssem.at[half], ici_rsem.at[d_group(half)], far)

    def pair_copy(k):
        return remote(my_piece(k), my_piece(k), pair_ssem.at[k], pair_rsem.at[k], partner)

    def pair_arrived(k):
        remote(my_piece(k), ubuf.at[spot(k, 1 - core)], pair_ssem.at[k], pair_rsem.at[k], partner).wait_recv()

    def ici_arrived(k):
        remote(my_piece(0), my_piece(k), x_ssem.at[0], ici_rsem.at[k], dev_x).wait_recv()

    for half in HALVES:
        x_copy(half).start()
        y_copy(half).start()
        pair_copy(half).start()

    def group_rows(k, cc):
        side = lax.rem(k, 2)
        is_own = (k < 2).astype(jnp.int32)
        is_diag = (k >= 6).astype(jnp.int32)
        is_side = 1 - is_own - is_diag
        side_chip = chips[1] * (1 - side) + chips[2] * side
        chip = chips[3] * is_own + chips[0] * is_diag + side_chip * is_side
        half = side * (1 - is_side) + ((k - 2) // 2) * is_side
        return pl.ds(pl.multiple_of(chip * 4 * piece + cc * 2 * piece + half * piece, 32), piece)

    def out_copy(k, cc, n):
        src = ubuf if n == n_stage else stage[n]
        return pltpu.make_async_copy(src.at[spot(k, cc)], res_hbm[n].at[group_rows(k, cc), :], out_sem.at[n, spot(k, cc)])

    def compute(j, first, count):
        four = pl.ds(first, count)
        left = ubuf[four].reshape(count * piece, ubuf.shape[2])
        for n, (start, size) in enumerate(qtiles):
            @pl.when(j == 0)
            def _():
                w_copy(n).wait()
            cols = slice(start, start + size)
            part = dot_nn(left, wq[:, cols]).astype(BF16)
            stage[0][four, :, cols] = part.reshape(count, piece, size)
        for t in range(ftiles):
            @pl.when(j == 0)
            def _():
                w_copy(len(qtiles) + 2 * t).wait()
                w_copy(len(qtiles) + 2 * t + 1).wait()
            cols = slice(t * WIDE, (t + 1) * WIDE)
            gate = dot_nn(left, wg[:, cols]).astype(BF16)
            up = dot_nn(left, wu[:, cols]).astype(BF16)
            stage[1][four, :, cols] = gate.reshape(count, piece, WIDE)
            stage[2][four, :, cols] = up.reshape(count, piece, WIDE)
            if with_hidden:
                hid = gated(gate.astype(F32), up.astype(F32)).astype(BF16)
                stage[3][four, :, cols] = hid.reshape(count, piece, WIDE)
        for n in range(n_res):
            for i in range(count):
                out_copy(first // 2 + i // 2, i % 2, n).start()

    def pass_on(k):
        ici_arrived(k)
        pair_copy(k).start()

    def step(j):
        for half in HALVES:
            @pl.when(j == half + 1)
            def _():
                pass_on(x_group(half))

                @pl.when(core == 0)
                def _():
                    fwd_copy(half).start()
                pass_on(y_group(half))

                @pl.when(core == 1)
                def _():
                    fwd_copy(half).start()
        for half in HALVES:
            pair_arrived(2 * j + half)
        compute(j, 4 * j, 4)

    loop(3, step)

    def diag_step(half):
        k = d_group(half)
        pass_on(k)
        pair_arrived(k)
        compute(k, 2 * k, 2)

    loop(2, diag_step)

    for half in HALVES:
        x_copy(half).wait_send()
        y_copy(half).wait_send()
        fwd_copy(half).wait_send()

    def drain(k):
        pair_copy(k).wait_send()
        for cc in HALVES:
            for n in range(n_res):
                out_copy(k, cc, n).wait()

    loop(8, drain)


def gather_project(x_loc, total, gain_row, w_qkv, w_gate, w_up, layer, with_hidden, with_u, tp_axis, tp_size, cid):
    rows, d_model = x_loc.shape
    seq = rows * tp_size
    piece = rows // 2
    qcols, fcols = w_qkv.shape[2], w_gate.shape[2]
    with_total = total is not None
    vmem = pl.BlockSpec(memory_space=pltpu.VMEM)
    hbm = pl.BlockSpec(memory_space=pl.ANY)
    widths = [qcols, fcols, fcols] + [fcols] * with_hidden + [d_model] * with_u
    stage_widths = widths[:3 + with_hidden]
    n_w = -(-qcols // WIDE) + 2 * (fcols // WIDE)
    dma = pltpu.SemaphoreType.DMA
    local = jax.ShapeDtypeStruct((rows, d_model), BF16)
    return pl.pallas_call(
        functools.partial(ag_body, layer, with_total, with_hidden, with_u, tp_axis),
        in_specs=[vmem] * (2 + with_total) + [hbm] * 3,
        out_specs=[vmem] * (1 + with_total) + [hbm] * len(widths),
        out_shape=[local] * (1 + with_total) + [jax.ShapeDtypeStruct((seq, w), BF16) for w in widths],
        scratch_shapes=[pltpu.VMEM((d_model, qcols), BF16), pltpu.VMEM((d_model, fcols), BF16), pltpu.VMEM((d_model, fcols), BF16), pltpu.VMEM((2 * tp_size, piece, d_model), BF16)]
        + [pltpu.VMEM((2 * tp_size, piece, w), BF16) for w in stage_widths]
        + [dma((n_w,)), dma((2,)), dma((2,)), dma((8,)), dma((2,)), dma((8,)), dma((8,)), dma((len(widths), 16))],
        compiler_params=pltpu.CompilerParams(collective_id=cid, has_side_effects=True, vmem_limit_bytes=VMEM_MAX),
        cost_estimate=pl.CostEstimate(flops=4 * seq * d_model * (qcols + 2 * fcols), bytes_accessed=40 * 2 ** 20, transcendentals=0),
        name="ag_project",
    )(*([x_loc] + ([total] if with_total else []) + [gain_row, w_qkv, w_gate, w_up]))


def gain_body(tp_axis, tp_size, in_ref, out_ref, slots, ssem, rsem):
    me = lax.axis_index(tp_axis)
    barrier = pltpu.get_barrier_semaphore()
    for k in range(1, tp_size):
        pl.semaphore_signal(barrier, inc=1, device_id={tp_axis: lax.rem(me + k, tp_size)}, device_id_type=pl.DeviceIdType.MESH)
    pl.semaphore_wait(barrier, tp_size - 1)
    slots[me] = in_ref[...]
    copies = []
    for k in range(1, tp_size):
        copies.append(pltpu.make_async_remote_copy(src_ref=in_ref, dst_ref=slots.at[me], send_sem=ssem.at[k], recv_sem=rsem.at[k], device_id={tp_axis: lax.rem(me + k, tp_size)}, device_id_type=pl.DeviceIdType.MESH))
        copies[-1].start()
    for k in range(1, tp_size):
        source = lax.rem(me + tp_size - k, tp_size)
        pltpu.make_async_remote_copy(src_ref=in_ref, dst_ref=slots.at[source], send_sem=ssem.at[k], recv_sem=rsem.at[k], device_id={tp_axis: source}, device_id_type=pl.DeviceIdType.MESH).wait_recv()
    total = slots[0]
    for k in range(1, tp_size):
        total = total + slots[k]
    out_ref[...] = total
    for copy in copies:
        copy.wait_send()


def sum_gains(part, tp_axis, tp_size, cid):
    return pl.pallas_call(
        functools.partial(gain_body, tp_axis, tp_size),
        in_specs=[pl.BlockSpec(memory_space=pltpu.VMEM)],
        out_specs=pl.BlockSpec(memory_space=pltpu.VMEM),
        out_shape=jax.ShapeDtypeStruct(part.shape, F32),
        scratch_shapes=[pltpu.VMEM((tp_size,) + part.shape, F32), pltpu.SemaphoreType.DMA((tp_size,)), pltpu.SemaphoreType.DMA((tp_size,))],
        compiler_params=pltpu.CompilerParams(collective_id=cid, has_side_effects=True),
        name="gain_sum",
    )(part)


def solution(mesh):
    tp_size = mesh.shape['tp']
    row_spec = P(('dp', 'tp'), None)
    col_spec = P(None, None, 'tp')
    inner_spec = P(None, 'tp', None)

    def device_program(x_loc, dy_loc, norm_gain, w_qkv, w_out, w_gate, w_up, w_down):
        n_layers = w_qkv.shape[0]
        heads = w_out.shape[1] // HEAD_DIM
        hcols = heads * HEAD_DIM
        seq = x_loc.shape[0] * tp_size
        cos_tab, sin_tab = rope_tables(seq)
        gather = lambda value: lax.all_gather(value, 'tp', axis=0, tiled=True)
        saved = []
        x_cur, total = x_loc, None
        u_full = None
        dy_parts = []
        for layer in range(n_layers):
            last = layer == n_layers - 1
            results = list(gather_project(x_cur, total, norm_gain[layer:layer + 1], w_qkv, w_gate, w_up, layer, not last, last, 'tp', tp_size, 2 * n_layers + layer))
            if total is not None:
                x_cur = results.pop(0)
            u_loc, qkv, gate, up, extra = results
            if last:
                u_full = extra
            query, key, value, attn, lse, dy_part = attn_forward(qkv, cos_tab, sin_tab, dy_loc, heads, 'tp', 3 * n_layers + 1 + layer, layer, n_layers)
            dy_parts.append(dy_part)
            saved.append((x_cur, u_loc, query, key, value, attn, lse, gate, up))
            if not last:
                total, = matmul_reduce_scatter([attn, extra], [w_out, w_down], layer, False, 'tp', tp_size, layer)

        grads = [None] * 5
        gains = [None] * n_layers
        dy_cur = dy_loc
        for layer in reversed(range(n_layers)):
            x_sav, u_loc, query, key, value, attn, lse, gate, up = saved[layer]
            d_attn, d_gate, d_up, hidden = cotangents(dy_parts, w_out, w_down, gate, up, layer)
            d_qkv = attn_backward(query, d_attn, lse, key, value, cos_tab, sin_tab, heads)
            dy_cur, gains[layer], *ready = matmul_reduce_scatter([d_qkv, d_gate, d_up], [w_qkv, w_gate, w_up], layer, True, 'tp', tp_size, n_layers + layer, [u_full, x_sav, norm_gain[layer:layer + 1], dy_cur])
            dy_cur, attn, hidden, *rest = lax.optimization_barrier((dy_cur, attn, hidden, *ready, *dy_parts))
            ready, dy_parts = rest[:3], rest[3:]
            if layer > 0:
                dy_next = gather(dy_cur)
            grads = tail_grads(attn, hidden, dy_parts, ready, grads, layer, n_layers)
            if layer > 0:
                dy_next, u_next, *grads = lax.optimization_barrier((dy_next, saved[layer - 1][1], *grads))
                dy_parts = [dy_next]
                u_full = gather(u_next)
        grad_gain = sum_gains(jnp.concatenate(gains), 'tp', tp_size, 3 * n_layers)
        return (dy_cur, grad_gain, *grads)

    return jax.shard_map(device_program, mesh=mesh, in_specs=(row_spec, row_spec, P(None, None), col_spec, inner_spec, col_spec, col_spec, inner_spec), out_specs=(row_spec, P('dp', None), P('dp', None, 'tp'), P('dp', 'tp', None), P('dp', None, 'tp'), P('dp', None, 'tp'), P('dp', 'tp', None)), check_vma=False)
```

```python
import functools

import jax
import jax.numpy as jnp
import numpy as np
from jax import lax
from jax.experimental import pallas as pl
from jax.experimental.pallas import tpu as pltpu
from jax.sharding import PartitionSpec as P

HEAD_DIM = 128
NORM_EPS = 1e-5
ROPE_BASE = 10000.0
BF16 = jnp.bfloat16
F32 = jnp.float32
VMEM_MAX = 67043328


DIAG, XSIDE, YSIDE, SELF = range(4)
HALVES = range(2)
WHOLE = slice(None)


def loop(count, body):
    def step(i, carry):
        body(i)
        return carry

    lax.fori_loop(0, count, step, 0)


def take(refs, count):
    return [next(refs) for _ in range(count)]


def tile_ds(index, size):
    return pl.ds(pl.multiple_of(index * size, size), size)


def rope_tables(seq_len):
    half_dim = HEAD_DIM // 2
    freqs = ROPE_BASE ** (-2.0 * np.arange(half_dim) / HEAD_DIM)
    angles = np.arange(seq_len)[:, None] * freqs[None, :]
    cos, sin = np.cos(angles), np.sin(angles)
    tables = np.concatenate([cos, cos], axis=1), np.concatenate([-sin, sin], axis=1)
    return [jnp.asarray(table.astype(np.float32)) for table in tables]


def rms_scale(x_f32, gain_row):
    inv_rms = lax.rsqrt(jnp.mean(x_f32 * x_f32, axis=-1, keepdims=True) + NORM_EPS)
    return x_f32 * inv_rms * gain_row


def gated(gate_f32, up_f32):
    return jax.nn.silu(gate_f32) * up_f32


def dot_nt(lhs, rhs):
    return lax.dot_general(lhs, rhs, (((1,), (1,)), ((), ())), preferred_element_type=F32)


def dot_tn(lhs, rhs):
    return lax.dot_general(lhs, rhs, (((0,), (0,)), ((), ())), preferred_element_type=F32)


def dot_nn(lhs, rhs):
    return lax.dot_general(lhs, rhs, (((1,), (0,)), ((), ())), preferred_element_type=F32)


def turn(values, cos_tab, sin_tab):
    return values * cos_tab + pltpu.roll(values, HEAD_DIM // 2, 1) * sin_tab


def ring_ids(tp_axis):
    me = lax.axis_index(tp_axis)
    core = lax.rem(me, 2)
    chip = me // 2
    x = lax.rem(chip, 2)
    y = chip // 2
    chips = ((1 - y) * 2 + (1 - x), y * 2 + (1 - x), (1 - y) * 2 + x, chip)
    partner = chip * 2 + (1 - core)
    dev_x = chips[1] * 2 + core
    dev_y = chips[2] * 2 + core
    near = dev_x * (1 - core) + dev_y * core
    far = dev_y * (1 - core) + dev_x * core
    return core, chips, partner, dev_x, dev_y, near, far


def greet(tp_axis, others):
    barrier = pltpu.get_barrier_semaphore()
    for other in others:
        pl.semaphore_signal(barrier, device_id={tp_axis: other}, device_id_type=pl.DeviceIdType.MESH)
    pl.semaphore_wait(barrier, len(others))


def remote_copy(tp_axis, src, dst, ssem, rsem, target):
    return pltpu.make_async_remote_copy(src_ref=src, dst_ref=dst, send_sem=ssem, recv_sem=rsem, device_id={tp_axis: target}, device_id_type=pl.DeviceIdType.MESH)


def sum_over(tp_axis, tp_size, slots, ssem, rsem):
    me = lax.axis_index(tp_axis)
    mine = slots.at[me]
    others = range(1, tp_size)

    def pushed(k):
        return remote_copy(tp_axis, mine, mine, ssem.at[k], rsem.at[k], lax.rem(me + k, tp_size))

    for k in others:
        pushed(k).start()
    for k in others:
        source = lax.rem(me + tp_size - k, tp_size)
        remote_copy(tp_axis, mine, slots.at[source], ssem.at[k], rsem.at[k], source).wait_recv()
    total = slots[0]
    for k in others:
        total = total + slots[k]
    for k in others:
        pushed(k).wait_send()
    return total


class PushGather:
    def __init__(self, tp_axis, src, dst, sems):
        self.tp_axis, self.src, self.dst = tp_axis, src, dst
        self.near_sem, self.far_sem, self.fwd_sem, self.ici_sem, self.pair_ssem, self.pair_rsem, self.own_sem = sems
        self.core, self.chips, self.partner, self.dev_x, self.dev_y, self.near, self.far = ring_ids(tp_axis)
        self.rows = src.shape[0]
        near_chip = self.chips[1] * (1 - self.core) + self.chips[2] * self.core
        far_chip = self.chips[2] * (1 - self.core) + self.chips[1] * self.core
        self.order = (self.chips[3], near_chip, far_chip, self.chips[0])

    def spot(self, chip, core):
        return self.dst.at[pl.ds(pl.multiple_of((chip * 2 + core) * self.rows, self.rows), self.rows), :]

    def remote(self, src, dst, ssem, rsem, target):
        return remote_copy(self.tp_axis, src, dst, ssem, rsem, target)

    def mine(self):
        return self.spot(self.chips[3], self.core)

    def near_copy(self):
        return self.remote(self.src, self.mine(), self.near_sem, self.ici_sem.at[1], self.near)

    def far_copy(self):
        return self.remote(self.src, self.mine(), self.far_sem, self.ici_sem.at[2], self.far)

    def fwd_copy(self):
        block = self.spot(self.order[1], self.core)
        return self.remote(block, block, self.fwd_sem, self.ici_sem.at[3], self.far)

    def pair_copy(self, k):
        block = self.spot(self.order[k], self.core)
        return self.remote(self.src if k == 0 else block, block, self.pair_ssem.at[k], self.pair_rsem.at[self.slot(k)], self.partner)

    def slot(self, k):
        return (0, 2, 1, 3)[k]

    def own_copy(self):
        return pltpu.make_async_copy(self.src, self.mine(), self.own_sem)

    def start(self):
        greet(self.tp_axis, (self.partner, self.dev_x, self.dev_y))
        self.near_copy().start()
        self.far_copy().start()
        self.pair_copy(0).start()
        self.own_copy().start()

    def ici_arrived(self, k):
        block = self.spot(self.order[k], self.core)
        self.remote(self.src, block, self.near_sem, self.ici_sem.at[k], self.near).wait_recv()

    def pass_sides(self):
        self.ici_arrived(1)
        self.fwd_copy().start()
        self.pair_copy(1).start()
        self.ici_arrived(2)
        self.pair_copy(2).start()

    def finish(self):
        self.ici_arrived(3)
        self.pair_copy(3).start()
        self.own_copy().wait()
        self.near_copy().wait_send()
        self.far_copy().wait_send()
        self.fwd_copy().wait_send()
        for k in range(4):
            self.pair_copy(k).wait_send()
            block = self.spot(self.order[k], 1 - self.core)
            self.remote(self.src, block, self.pair_ssem.at[k], self.pair_rsem.at[k], self.partner).wait_recv()


    def open(self, step):
        @pl.when(step == 0)
        def _():
            self.start()

        @pl.when(step == pl.num_programs(0) - 1)
        def _():
            self.pass_sides()

    def close(self, step):
        @pl.when(step == pl.num_programs(0) - 1)
        def _():
            self.finish()


class NoPush:
    n_refs, specs, shapes, sems, params, operands = 0, [], [], [], {}, []

    def __call__(self, src, dst, sems):
        return self

    def open(self, step):
        pass

    close = open


class PushOf:
    n_refs = 1

    def __init__(self, value, part, n_parts, tp_axis, tp_size, cid):
        self.tp_axis = tp_axis
        rows, self.width = value.shape[0], value.shape[1] // n_parts
        self.cols = slice(part * self.width, (part + 1) * self.width)
        dma = pltpu.SemaphoreType.DMA
        self.operands = [value]
        self.specs = [pl.BlockSpec(memory_space=pl.ANY)]
        self.shapes = [jax.ShapeDtypeStruct((rows * tp_size, self.width), BF16)]
        self.sems = [dma(())] * 3 + [dma((4,))] * 3 + [dma(())]
        self.params = {'collective_id': cid, 'has_side_effects': True}

    def __call__(self, src, dst, sems):
        return PushGather(self.tp_axis, src[0].at[:, self.cols], dst[0], list(sems))


def fold(values, op):
    acc = values[:, :HEAD_DIM]
    for at in range(HEAD_DIM, values.shape[1], HEAD_DIM):
        acc = op(acc, values[:, at:at + HEAD_DIM])
    return acc


def attn_fwd_body(heads, blk, push_of, qkv_ref, cos_ref, sin_ref, v_ref, dy_hbm, q_out, k_out, v_out, o_out, lse_out, dy_full, score_buf, k_rot, *sems):
    step = pl.program_id(0)
    push = push_of([dy_hbm], [dy_full], sems)
    push.open(step)
    scale = HEAD_DIM ** -0.5
    kcol = heads * HEAD_DIM
    vcol = kcol + HEAD_DIM
    cos_tab, sin_tab = cos_ref[...], sin_ref[...]
    here = tile_ds(step, blk)
    key = turn(qkv_ref[:, kcol:vcol].astype(F32), cos_tab, sin_tab).astype(BF16)
    k_rot[here, :] = key
    k_out[...] = key
    v_out[...] = qkv_ref[:, vcol:]
    parts = []
    for head in range(heads):
        cols = slice(head * HEAD_DIM, (head + 1) * HEAD_DIM)
        part = turn(qkv_ref[:, cols].astype(F32), cos_tab, sin_tab).astype(BF16)
        q_out[:, cols] = part
        parts.append(part)
    query = jnp.concatenate(parts, axis=0)
    rows = heads * blk

    diag = dot_nt(query, key) * scale
    row_id = lax.broadcasted_iota(jnp.int32, (heads, blk, blk), 1).reshape(rows, blk)
    col_id = lax.broadcasted_iota(jnp.int32, (rows, blk), 1)
    diag = jnp.where(row_id >= col_id, diag, -1e30)
    top = fold(diag, jnp.maximum)

    def first(j, top):
        there = tile_ds(j, blk)
        score = dot_nt(query, k_rot[there, :]) * scale
        score_buf[j] = score
        return jnp.maximum(top, fold(score, jnp.maximum))

    top = jnp.max(lax.fori_loop(0, step, first, top), axis=-1, keepdims=True)

    diag = jnp.exp(diag - top)
    total = fold(diag, jnp.add)

    def second(j, total):
        prob = jnp.exp(score_buf[j] - top)
        score_buf[j] = prob
        return total + fold(prob, jnp.add)

    total = jnp.sum(lax.fori_loop(0, step, second, total), axis=-1, keepdims=True)
    inv = 1.0 / total
    acc = dot_nn((diag * inv).astype(BF16), v_ref[here, :])

    def third(j, acc):
        there = tile_ds(j, blk)
        return acc + dot_nn((score_buf[j] * inv).astype(BF16), v_ref[there, :])

    acc = lax.fori_loop(0, step, third, acc)
    lse = top + jnp.log(total)
    lane = lax.broadcasted_iota(jnp.int32, (blk, HEAD_DIM), 1)
    packed = jnp.zeros((blk, HEAD_DIM), F32)
    for head in range(heads):
        rws = slice(head * blk, (head + 1) * blk)
        o_out[:, head * HEAD_DIM:(head + 1) * HEAD_DIM] = acc[rws].astype(BF16)
        packed = jnp.where(lane == head, lse[rws], packed)
    lse_out[...] = packed
    push.close(step)


def attn_forward(qkv, cos_tab, sin_tab, heads, push_of, blk=384):
    seq, width = qkv.shape
    hcols = heads * HEAD_DIM
    steps = seq // blk
    row = lambda i: (i, 0)
    flops = 4 * heads * seq * seq * HEAD_DIM // 2
    return pl.pallas_call(
        functools.partial(attn_fwd_body, heads, blk, push_of),
        grid=(steps,),
        in_specs=[pl.BlockSpec((blk, width), row), pl.BlockSpec((blk, HEAD_DIM), row), pl.BlockSpec((blk, HEAD_DIM), row), pl.BlockSpec((seq, HEAD_DIM), lambda i: (0, heads + 1))] + push_of.specs,
        out_specs=[pl.BlockSpec((blk, hcols), row), pl.BlockSpec((blk, HEAD_DIM), row), pl.BlockSpec((blk, HEAD_DIM), row), pl.BlockSpec((blk, hcols), row), pl.BlockSpec((blk, HEAD_DIM), row)] + push_of.specs,
        out_shape=[jax.ShapeDtypeStruct((seq, hcols), BF16), jax.ShapeDtypeStruct((seq, HEAD_DIM), BF16), jax.ShapeDtypeStruct((seq, HEAD_DIM), BF16), jax.ShapeDtypeStruct((seq, hcols), BF16), jax.ShapeDtypeStruct((seq, HEAD_DIM), F32)] + push_of.shapes,
        scratch_shapes=[pltpu.VMEM((steps, heads * blk, blk), F32), pltpu.VMEM((seq, HEAD_DIM), BF16)] + push_of.sems,
        compiler_params=pltpu.CompilerParams(**push_of.params, dimension_semantics=("arbitrary",), vmem_limit_bytes=VMEM_MAX),
        cost_estimate=pl.CostEstimate(flops=flops * 4, bytes_accessed=8 * 2 ** 20, transcendentals=heads * seq * seq // 2),
        name="attn_fwd",
    )(qkv, cos_tab, sin_tab, qkv, *push_of.operands)


def attn_bwd_body(heads, blk, push_of, q_ref, do_ref, lse_ref, k_ref, v_ref, cos_ref, sin_ref, *refs):
    refs = iter(refs)
    src = take(refs, push_of.n_refs)
    out_ref = next(refs)
    dst = take(refs, push_of.n_refs)
    prob_buf, dprob_buf, dk_acc, dv_acc = take(refs, 4)
    push = push_of(src, dst, refs)
    step = pl.program_id(0)
    push.open(step)
    scale = HEAD_DIM ** -0.5
    rows = heads * blk
    hcols = heads * HEAD_DIM
    here = tile_ds(step, blk)

    @pl.when(step == 0)
    def _():
        dk_acc[...] = jnp.zeros_like(dk_acc)
        dv_acc[...] = jnp.zeros_like(dv_acc)

    def heads_of(ref):
        return jnp.concatenate([ref[:, h * HEAD_DIM:(h + 1) * HEAD_DIM] for h in range(heads)], axis=0)

    query = heads_of(q_ref)
    d_out = heads_of(do_ref)
    lse = jnp.concatenate([lse_ref[:, h:h + 1] for h in range(heads)], axis=0)
    row_id = lax.broadcasted_iota(jnp.int32, (heads, blk, blk), 1).reshape(rows, blk)
    col_id = lax.broadcasted_iota(jnp.int32, (rows, blk), 1)

    def score_part(j, masked):
        there = tile_ds(j, blk)
        score = dot_nt(query, k_ref[there, :]) * scale
        if masked:
            score = jnp.where(row_id >= col_id, score, -1e30)
        prob = jnp.exp(score - lse)
        d_prob = dot_nt(d_out, v_ref[there, :]).astype(BF16)
        prob_buf[j] = prob
        dprob_buf[j] = d_prob
        dv_acc[there, :] += dot_tn(prob.astype(BF16), d_out)
        return fold(prob * d_prob.astype(F32), jnp.add)

    row_dot = score_part(step, True)
    row_dot = lax.fori_loop(0, step, lambda j, tot: tot + score_part(j, False), row_dot)
    row_dot = jnp.sum(row_dot, axis=-1, keepdims=True)

    def grad_part(j, acc):
        there = tile_ds(j, blk)
        d_score = (prob_buf[j] * (dprob_buf[j].astype(F32) - row_dot) * scale).astype(BF16)
        dk_acc[there, :] += dot_tn(d_score, query)
        return acc + dot_nn(d_score, k_ref[there, :])

    d_query = lax.fori_loop(0, step + 1, grad_part, jnp.zeros((rows, HEAD_DIM), F32))
    cos_tab, sin_tab = cos_ref[here, :], sin_ref[here, :]
    for head in range(heads):
        part = d_query[head * blk:(head + 1) * blk].astype(BF16).astype(F32)
        out_ref[here, head * HEAD_DIM:(head + 1) * HEAD_DIM] = turn(part, cos_tab, -sin_tab).astype(BF16)

    @pl.when(step == pl.num_programs(0) - 1)
    def _():
        d_key = dk_acc[...].astype(BF16).astype(F32)
        out_ref[:, hcols:hcols + HEAD_DIM] = turn(d_key, cos_ref[...], -sin_ref[...]).astype(BF16)
        out_ref[:, hcols + HEAD_DIM:] = dv_acc[...].astype(BF16)

    push.close(step)


def attn_backward(query, d_attn, lse, key, value, cos_tab, sin_tab, heads, push_of, blk=384):
    seq = query.shape[0]
    hcols = heads * HEAD_DIM
    width = hcols + 2 * HEAD_DIM
    steps = seq // blk
    row = lambda i: (i, 0)
    whole = lambda i: (0, 0)
    flops = 10 * heads * seq * seq * HEAD_DIM // 2
    return pl.pallas_call(
        functools.partial(attn_bwd_body, heads, blk, push_of),
        grid=(steps,),
        in_specs=[pl.BlockSpec((blk, hcols), row), pl.BlockSpec((blk, hcols), row), pl.BlockSpec((blk, HEAD_DIM), row)] + [pl.BlockSpec((seq, HEAD_DIM), whole)] * 4 + push_of.specs,
        out_specs=[pl.BlockSpec((seq, width), whole)] + push_of.specs,
        out_shape=[jax.ShapeDtypeStruct((seq, width), BF16)] + push_of.shapes,
        scratch_shapes=[pltpu.VMEM((steps, heads * blk, blk), F32), pltpu.VMEM((steps, heads * blk, blk), BF16), pltpu.VMEM((seq, HEAD_DIM), F32), pltpu.VMEM((seq, HEAD_DIM), F32)] + push_of.sems,
        compiler_params=pltpu.CompilerParams(**push_of.params, dimension_semantics=("arbitrary",), vmem_limit_bytes=VMEM_MAX),
        cost_estimate=pl.CostEstimate(flops=flops * 4, bytes_accessed=10 * 2 ** 20, transcendentals=heads * seq * seq // 2),
        name="attn_bwd",
    )(query, d_attn, lse, key, value, cos_tab, sin_tab, *push_of.operands)


def dgrad_body(n_parts, push_of, *refs):
    refs = iter(refs)
    parts = take(refs, n_parts)
    wo_ref, wd_ref, gate_ref, up_ref = take(refs, 4)
    src = take(refs, push_of.n_refs)
    dattn_ref, dgate_ref, dup_ref, hid_ref = take(refs, 4)
    push = push_of(src, take(refs, push_of.n_refs), refs)
    push.open(pl.program_id(0))

    def product(w_ref, rows):
        acc, at = None, 0
        for part in parts:
            width = part.shape[1]
            term = dot_nt(part[...], w_ref[0, rows, at:at + width])
            acc = term if acc is None else acc + term
            at += width
        return acc.astype(BF16)

    dattn_ref[...] = product(wo_ref, slice(None))
    for t in range(gate_ref.shape[1] // BROAD):
        cols = slice(t * BROAD, (t + 1) * BROAD)
        d_hidden = product(wd_ref, cols)
        hidden, pull = jax.vjp(gated, gate_ref[:, cols].astype(F32), up_ref[:, cols].astype(F32))
        d_gate, d_up = pull(d_hidden.astype(F32))
        hid_ref[:, cols] = hidden.astype(BF16)
        dgate_ref[:, cols] = d_gate.astype(BF16)
        dup_ref[:, cols] = d_up.astype(BF16)
    push.close(pl.program_id(0))


def cotangents(dy_parts, w_out, w_down, gate, up, layer, push_of, blk=512):
    seq, fcols = gate.shape
    hcols, d_model = w_out.shape[1:]
    row = lambda i: (i, 0)
    flops = 2 * seq * d_model * (hcols + fcols)
    wide = pl.BlockSpec((blk, fcols), row)
    return pl.pallas_call(
        functools.partial(dgrad_body, len(dy_parts), push_of),
        grid=(seq // blk,),
        in_specs=[pl.BlockSpec((blk, part.shape[1]), row) for part in dy_parts] + [pl.BlockSpec((1, hcols, d_model), lambda i: (layer, 0, 0)), pl.BlockSpec((1, fcols, d_model), lambda i: (layer, 0, 0)), wide, wide] + push_of.specs,
        out_specs=[pl.BlockSpec((blk, hcols), row), wide, wide, wide] + push_of.specs,
        out_shape=[jax.ShapeDtypeStruct((seq, hcols), BF16)] + [jax.ShapeDtypeStruct((seq, fcols), BF16)] * 3 + push_of.shapes,
        scratch_shapes=push_of.sems,
        compiler_params=pltpu.CompilerParams(**push_of.params, dimension_semantics=("arbitrary",), vmem_limit_bytes=VMEM_MAX),
        cost_estimate=pl.CostEstimate(flops=flops, bytes_accessed=32 * 2 ** 20, transcendentals=seq * fcols),
        name="cotangents",
    )(*dy_parts, w_out, w_down, gate, up, *push_of.operands)


def spans(parts, blk):
    result, begin = [], 0
    for part in parts:
        end = begin + part.shape[1] // blk
        result.append((begin, end - 1))
        begin = end
    return result


def on_part(step, ranges, parts, body):
    for (begin, last), part in zip(ranges, parts):
        @pl.when(jnp.logical_and(step >= begin, step <= last))
        def _():
            body(part[...])


def tail_body(dy_spans, u_spans, *refs):
    refs = iter(refs)
    attn_ref, hid_ref = take(refs, 2)
    parts = take(refs, len(dy_spans))
    u_parts = take(refs, len(u_spans))
    q_ref, g_ref, u_ref = take(refs, 3)
    q_out, out_out, g_out, u_out, down_out = list(refs)[-5:]
    step = pl.program_id(0)

    def from_dy(right):
        out_out[0] = dot_tn(attn_ref[...], right).astype(BF16)
        down_out[0] = dot_tn(hid_ref[...], right).astype(BF16)

    def from_u(left):
        q_out[0] = dot_tn(left, q_ref[...]).astype(BF16)

    on_part(step, dy_spans, parts, from_dy)
    if u_spans:
        on_part(step, u_spans, u_parts, from_u)
    else:
        q_out[0] = q_ref[...]
    g_out[0] = g_ref[...]
    u_out[0] = u_ref[...]


def tail_grads(attn, hidden, dy_parts, u_parts, ready, grads, layer, n_layers, blk=512):
    seq = attn.shape[0]
    d_model = sum(part.shape[1] for part in dy_parts)
    whole = lambda j: (0, 0)
    hbm = pl.BlockSpec(memory_space=pl.ANY)
    rows = lambda width: pl.BlockSpec((blk, width), lambda j: (j, 0))
    rows_out = lambda width: pl.BlockSpec((1, blk, width), lambda j: (layer, j, 0))
    cols_out = lambda height: pl.BlockSpec((1, height, blk), lambda j: (layer, 0, j))

    dy_spans, u_spans = spans(dy_parts, blk), spans(u_parts, blk)

    def part_specs(ranges):
        return [pl.BlockSpec((seq, blk), lambda j, begin=begin, last=last: (0, jnp.clip(j, begin, last) - begin)) for begin, last in ranges]

    hcols, fcols = attn.shape[1], hidden.shape[1]
    widths = [item.shape[1] for item in ready]
    old = [item for item in grads if item is not None]
    before = 5 + len(dy_parts) + len(u_parts)
    q_spec = pl.BlockSpec((seq, widths[0]), whole) if u_parts else rows(widths[0])
    return pl.pallas_call(
        functools.partial(tail_body, dy_spans, u_spans),
        grid=(d_model // blk,),
        in_specs=[pl.BlockSpec((seq, hcols), whole), pl.BlockSpec((seq, fcols), whole)] + part_specs(dy_spans + u_spans) + [q_spec] + [rows(w) for w in widths[1:]] + [hbm] * len(old),
        out_specs=[rows_out(widths[0]), cols_out(hcols), rows_out(widths[1]), rows_out(widths[2]), cols_out(fcols)],
        out_shape=[jax.ShapeDtypeStruct((n_layers,) + dims, BF16) for dims in ((d_model, widths[0]), (hcols, d_model), (d_model, widths[1]), (d_model, widths[2]), (fcols, d_model))],
        input_output_aliases={before + n: n for n in range(len(old))},
        compiler_params=pltpu.CompilerParams(dimension_semantics=("arbitrary",), vmem_limit_bytes=VMEM_MAX),
        cost_estimate=pl.CostEstimate(flops=2 * seq * d_model * (hcols + fcols), bytes_accessed=60 * 2 ** 20, transcendentals=0),
        name="tail_grads",
    )(attn, hidden, *dy_parts, *u_parts, *ready, *old)


TILE = 256
WIDE = 512
BROAD = 1024
NORM_ROWS = 32


def fill_weight_grads(fill_ops, u_parts, grads, lhs, rhs, sems):
    load_sem, store_sem = sems
    seq = u_parts[0].shape[0]

    def rows_at(base, slot):
        return pl.ds(pl.multiple_of(base + slot * TILE, TILE), TILE)

    def spots(slot):
        places = (rhs[0].at[rows_at(seq, slot), :], rhs[1].at[rows_at(seq, slot), :], rhs[1].at[rows_at(seq + WIDE, slot), :])
        return [places[i] for i in fill_ops]

    def one_part(begin, steps, u_hbm):
        def load(j, slot):
            return pltpu.make_async_copy(u_hbm.at[:, tile_ds(j, TILE)], rhs[2].at[0:seq, tile_ds(slot, TILE)], load_sem.at[slot])

        def stores(j, slot):
            return [pltpu.make_async_copy(src, dst.at[tile_ds(begin + j, TILE), :], store_sem.at[slot, k]) for k, (src, dst) in enumerate(zip(spots(slot), grads))]

        load(0, 0).start()

        def step(j):
            slot = lax.rem(j, 2)
            load(j, slot).wait()

            @pl.when(j + 1 < steps)
            def _():
                load(j + 1, 1 - slot).start()

            @pl.when(j >= 2)
            def _():
                for copy in stores(j - 2, slot):
                    copy.wait()
            left = rhs[2][0:seq, tile_ds(slot, TILE)]
            for spot, i in zip(spots(slot), fill_ops):
                spot[...] = dot_tn(left, lhs[i][...]).astype(BF16)
            for copy in stores(j, slot):
                copy.start()

        loop(steps, step)
        for j in (steps - 2, steps - 1):
            for copy in stores(j, j % 2):
                copy.wait()

    begin = 0
    for u_hbm in u_parts:
        steps = u_hbm.shape[1] // TILE
        one_part(begin, steps, u_hbm)
        begin += steps


def rs_body(n_ops, layer, trans, back, fill_ops, tp_size, tp_axis, *refs):
    refs = iter(refs)
    lhs_hbm = take(refs, n_ops)
    rhs_hbm = take(refs, n_ops)
    if back:
        u_hbm = take(refs, back)
        x_ref, gain_ref, dy_ref = take(refs, 3)
        if tp_size:
            above_ref = next(refs)
        dy_out, gain_out = take(refs, 2)
        grad_hbm = take(refs, len(fill_ops))
    out_ref = next(refs)
    lhs = take(refs, n_ops)
    rhs = take(refs, n_ops)
    (own, stage, pair_in, diag_in, near_in, far_in, last_out, last_in,
     lhs_sem, rhs_sem, pair_ssem, pair_rsem, diag_ssem, diag_rsem, near_ssem, near_rsem, far_ssem, far_rsem, last_ssem, last_rsem) = take(refs, 20)
    if tp_size:
        slots, slot_ssem, slot_rsem = take(refs, 3)
    fill_sems = list(refs)
    tiles, rblk = own.shape[1:3]
    rows_out = rblk // 2
    core, chips, partner, dev_x, dev_y, near, far = ring_ids(tp_axis)
    other = 1 - core
    near_slot = XSIDE + core
    far_slot = YSIDE - core

    def row_ds(slot):
        return tile_ds(chips[slot], rblk)

    def own_ds(t):
        return tile_ds(core * tiles + t, TILE)

    def pair_ds(t):
        return tile_ds(other * tiles + t, TILE)

    def lhs_copy(i, slot):
        return pltpu.make_async_copy(lhs_hbm[i].at[row_ds(slot), :], lhs[i].at[row_ds(slot), :], lhs_sem.at[i, slot])

    def rhs_copy(i, cols, which, t):
        if trans:
            return pltpu.make_async_copy(rhs_hbm[i].at[layer, cols, :], rhs[i].at[cols, :], rhs_sem.at[i, which, t])
        return pltpu.make_async_copy(rhs_hbm[i].at[layer, :, cols], rhs[i].at[:, cols], rhs_sem.at[i, which, t])

    def pair_load(i, t):
        return rhs_copy(i, pair_ds(t), 0, t)

    def own_load(i, t):
        return rhs_copy(i, own_ds(t), 1, t)

    ops = range(n_ops)
    for i in ops:
        lhs_copy(i, DIAG).start()
    for t in range(tiles):
        for i in ops:
            pair_load(i, t).start()
        for i in ops:
            own_load(i, t).start()
    for slot in (XSIDE, YSIDE, SELF):
        for i in ops:
            lhs_copy(i, slot).start()

    if tp_size:
        me = lax.axis_index(tp_axis)
        greet(tp_axis, [lax.rem(me + k, tp_size) for k in range(1, tp_size)])
    else:
        greet(tp_axis, (partner, dev_x, dev_y))

    def product(slot, cols):
        acc = None
        for i in range(n_ops):
            left = lhs[i][row_ds(slot), :]
            part = dot_nt(left, rhs[i][cols, :]) if trans else dot_nn(left, rhs[i][:, cols])
            acc = part if acc is None else acc + part
        return acc

    remote = functools.partial(remote_copy, tp_axis)

    def spot(slot, t):
        return stage.at[t if slot in (DIAG, YSIDE) else tiles + t]

    def pair_copy(slot, t):
        return remote(spot(slot, t), pair_in.at[slot, t], pair_ssem.at[slot, t], pair_rsem.at[slot, t], partner)

    def pair_wait(slot, t):
        remote(stage.at[t], pair_in.at[slot, t], pair_ssem.at[slot, t], pair_rsem.at[slot, t], partner).wait_recv()

    def diag_copy(t):
        return remote(own.at[DIAG, t], diag_in.at[t], diag_ssem.at[t], diag_rsem.at[t], near)

    def near_copy(t):
        return remote(own.at[near_slot, t], near_in.at[t], near_ssem.at[t], near_rsem.at[t], near)

    def far_copy(t):
        return remote(own.at[far_slot, t], far_in.at[t], far_ssem.at[t], far_rsem.at[t], far)

    def last_copy(t):
        return remote(last_out.at[t], last_in.at[t], last_ssem.at[t], last_rsem.at[t], partner)

    def emit_pair(slot, t):
        spot(slot, t)[...] = product(slot, pair_ds(t))
        pair_copy(slot, t).start()

    for i in ops:
        lhs_copy(i, DIAG).wait()

    def finish_diag(t):
        pair_wait(DIAG, t)
        own[DIAG, t] += pair_in[DIAG, t]
        diag_copy(t).start()

    def lagged(finish, t):
        @pl.when(t == 0)
        def _():
            finish(t)

        @pl.when(t > 1)
        def _():
            finish(t - 1)

    def diag_step(t):
        for i in ops:
            pair_load(i, t).wait()
        emit_pair(DIAG, t)
        for i in ops:
            own_load(i, t).wait()
        own[DIAG, t] = product(DIAG, own_ds(t))
        lagged(finish_diag, t)

    loop(tiles, diag_step)
    finish_diag(tiles - 1)

    for slot in (XSIDE, YSIDE):
        for i in ops:
            lhs_copy(i, slot).wait()

    def finish_sides(t):
        pair_wait(near_slot, t)
        own[near_slot, t] += pair_in[near_slot, t]
        near_copy(t).start()
        pair_wait(far_slot, t)
        diag_copy(t).wait_recv()
        own[far_slot, t] += pair_in[far_slot, t] + diag_in[t]
        far_copy(t).start()

    def side_step(t):
        emit_pair(XSIDE, t)
        pair_copy(DIAG, t).wait_send()
        emit_pair(YSIDE, t)
        own[XSIDE, t] = product(XSIDE, own_ds(t))
        own[YSIDE, t] = product(YSIDE, own_ds(t))
        lagged(finish_sides, t)

    loop(tiles, side_step)
    finish_sides(tiles - 1)

    for i in ops:
        lhs_copy(i, SELF).wait()

    def self_step(t):
        pair_copy(XSIDE, t).wait_send()
        emit_pair(SELF, t)
        own[SELF, t] = product(SELF, own_ds(t))

    loop(tiles, self_step)

    if back:
        fill_weight_grads(fill_ops, u_hbm, grad_hbm, lhs, rhs, fill_sems)

    def final_step(t):
        pair_wait(SELF, t)
        near_copy(t).wait_recv()
        own[SELF, t] += pair_in[SELF, t] + near_in[t]
        far_copy(t).wait_recv()
        own[SELF, t] += far_in[t]
        last_out[t] = own[SELF, t, tile_ds(other, rows_out), :]
        last_copy(t).start()
        out_ref[:, own_ds(t)] = own[SELF, t, tile_ds(core, rows_out), :]

    loop(tiles, final_step)

    def close_step(t):
        last_copy(t).wait_recv()
        out_ref[:, pair_ds(t)] = last_in[t]
        for copy in (pair_copy(YSIDE, t), pair_copy(SELF, t), diag_copy(t), near_copy(t), far_copy(t), last_copy(t)):
            copy.wait_send()

    loop(tiles, close_step)

    if back:
        gain = gain_ref[...]
        gain_sum = slots.at[me, 0:1, :] if tp_size else gain_out
        gain_sum[...] = jnp.zeros_like(gain)

        def norm_step(r):
            rows = tile_ds(r, NORM_ROWS)
            pull = jax.vjp(rms_scale, x_ref[rows, :].astype(F32), gain)[1]
            d_x, d_gain = pull(out_ref[rows, :].astype(BF16).astype(F32))
            dy_out[rows, :] = (dy_ref[rows, :].astype(F32) + d_x).astype(BF16)
            gain_sum[...] += d_gain

        loop(rows_out // NORM_ROWS, norm_step)
        if tp_size:
            slots[me, 1:, :] = above_ref[...]
            gain_out[...] = sum_over(tp_axis, tp_size, slots, slot_ssem, slot_rsem)


def matmul_reduce_scatter(lhs_list, rhs_list, layer, trans, tp_axis, tp_size, cid, u_parts=(), norm=(), fill_ops=(), n_gains=1):
    n_ops = len(lhs_list)
    seq = lhs_list[0].shape[0]
    d_model = rhs_list[0].shape[1] if trans else rhs_list[0].shape[2]
    rblk = seq * 2 // tp_size
    tiles = d_model // 2 // TILE
    rows_out = seq // tp_size
    ks = [item.shape[1] for item in lhs_list]
    dma = pltpu.SemaphoreType.DMA
    scratch = [pltpu.VMEM((seq, k), BF16) for k in ks]
    scratch += [pltpu.VMEM((d_model, k) if trans else (k, d_model), BF16) for k in ks]
    scratch += [
        pltpu.VMEM((4, tiles, rblk, TILE), F32),
        pltpu.VMEM((2 * tiles, rblk, TILE), F32),
        pltpu.VMEM((4, tiles, rblk, TILE), F32),
        pltpu.VMEM((tiles, rblk, TILE), F32),
        pltpu.VMEM((tiles, rblk, TILE), F32),
        pltpu.VMEM((tiles, rblk, TILE), F32),
        pltpu.VMEM((tiles, rows_out, TILE), F32),
        pltpu.VMEM((tiles, rows_out, TILE), F32),
        dma((n_ops, 4)), dma((n_ops, 2, tiles)),
        dma((4, tiles)), dma((4, tiles)),
    ] + [dma((tiles,))] * 8
    flops = 2 * seq * d_model * sum(ks)
    hbm = pl.BlockSpec(memory_space=pl.ANY)
    vmem = pl.BlockSpec(memory_space=pltpu.VMEM)
    operands = list(lhs_list) + list(rhs_list)
    in_specs = [hbm] * len(operands)
    out_specs, out_shape = [vmem], [jax.ShapeDtypeStruct((rows_out, d_model), F32)]
    if u_parts:
        operands += u_parts + norm
        in_specs += [hbm] * len(u_parts) + [vmem] * len(norm)
        scratch = [pltpu.VMEM((rows_out, d_model), F32)] + scratch
        if n_gains > 1:
            scratch += [pltpu.VMEM((tp_size, n_gains, d_model), F32), dma((tp_size,)), dma((tp_size,))]
        scratch += [dma((2,)), dma((2, 3))]
        out_specs = [vmem] * 2 + [hbm] * len(fill_ops)
        out_shape = [jax.ShapeDtypeStruct((rows_out, d_model), BF16), jax.ShapeDtypeStruct((n_gains, d_model), F32)]
        out_shape += [jax.ShapeDtypeStruct((d_model, ks[i]), BF16) for i in fill_ops]
    return pl.pallas_call(
        functools.partial(rs_body, n_ops, layer, trans, len(u_parts), fill_ops, tp_size if n_gains > 1 else 0, tp_axis),
        in_specs=in_specs,
        out_specs=out_specs,
        out_shape=out_shape,
        scratch_shapes=scratch,
        compiler_params=pltpu.CompilerParams(collective_id=cid, has_side_effects=True, vmem_limit_bytes=VMEM_MAX),
        cost_estimate=pl.CostEstimate(flops=flops * 3, bytes_accessed=40 * 2 ** 20, transcendentals=0),
        name="matmul_rs",
    )(*operands)


def ag_body(layer, with_total, with_hidden, with_u, tp_axis, *refs):
    refs = iter(refs)
    n_stage = 3 + with_hidden
    n_res = n_stage + with_u
    x_ref = next(refs)
    if with_total:
        total_ref = next(refs)
    gain_ref, wq_hbm, wg_hbm, wu_hbm = take(refs, 4)
    if with_total:
        x_out = next(refs)
    u_out = next(refs)
    res_hbm = take(refs, n_res)
    wq, wg, wu, ubuf = take(refs, 4)
    stage = take(refs, n_stage)
    w_sem, x_ssem, y_ssem, ici_rsem, fwd_ssem, pair_ssem, pair_rsem, out_sem = refs
    piece = ubuf.shape[1]

    core, chips, partner, dev_x, dev_y, near, far = ring_ids(tp_axis)
    qcols = wq.shape[1]
    fcols = wg.shape[1]
    qtiles = [(s, min(BROAD, qcols - s)) for s in range(0, qcols, BROAD)]
    ftiles = fcols // BROAD

    def w_copy(k):
        if k < len(qtiles):
            cols = slice(qtiles[k][0], qtiles[k][0] + qtiles[k][1])
            return pltpu.make_async_copy(wq_hbm.at[layer, :, cols], wq.at[:, cols], w_sem.at[k])
        t, which = divmod(k - len(qtiles), 2)
        cols = slice(t * BROAD, (t + 1) * BROAD)
        src, dst = ((wg_hbm, wg), (wu_hbm, wu))[which]
        return pltpu.make_async_copy(src.at[layer, :, cols], dst.at[:, cols], w_sem.at[k])

    n_w = len(qtiles) + 2 * ftiles
    for k in range(n_w):
        w_copy(k).start()

    def spot(group, cc):
        return group * 2 + cc

    gain = gain_ref[...]
    for half in HALVES:
        rows = tile_ds(half, piece)
        x_f32 = x_ref[rows, :].astype(F32)
        if with_total:
            x_new = (x_f32 + total_ref[rows, :]).astype(BF16)
            x_out[rows, :] = x_new
            x_f32 = x_new.astype(F32)
        u_new = rms_scale(x_f32, gain).astype(BF16)
        u_out[rows, :] = u_new
        ubuf[spot(half, core)] = u_new
    greet(tp_axis, (partner, dev_x, dev_y))

    remote = functools.partial(remote_copy, tp_axis)

    def x_group(half):
        return 2 + 2 * half

    def y_group(half):
        return 3 + 2 * half

    def d_group(half):
        return 6 + half

    def my_piece(group):
        return ubuf.at[spot(group, core)]

    def x_copy(half):
        return remote(my_piece(half), my_piece(x_group(half)), x_ssem.at[half], ici_rsem.at[x_group(half)], dev_x)

    def y_copy(half):
        return remote(my_piece(half), my_piece(y_group(half)), y_ssem.at[half], ici_rsem.at[y_group(half)], dev_y)

    def fwd_copy(half):
        return remote(my_piece(x_group(half) + core), my_piece(d_group(half)), fwd_ssem.at[half], ici_rsem.at[d_group(half)], far)

    def pair_copy(k):
        return remote(my_piece(k), my_piece(k), pair_ssem.at[k], pair_rsem.at[k], partner)

    def pair_arrived(k):
        remote(my_piece(k), ubuf.at[spot(k, 1 - core)], pair_ssem.at[k], pair_rsem.at[k], partner).wait_recv()

    def ici_arrived(k):
        remote(my_piece(0), my_piece(k), x_ssem.at[0], ici_rsem.at[k], dev_x).wait_recv()

    for half in HALVES:
        x_copy(half).start()
        y_copy(half).start()
        pair_copy(half).start()

    def group_rows(k, cc):
        side = lax.rem(k, 2)
        is_own = (k < 2).astype(jnp.int32)
        is_diag = (k >= 6).astype(jnp.int32)
        is_side = 1 - is_own - is_diag
        side_chip = chips[1] * (1 - side) + chips[2] * side
        chip = chips[3] * is_own + chips[0] * is_diag + side_chip * is_side
        half = side * (1 - is_side) + ((k - 2) // 2) * is_side
        return pl.ds(pl.multiple_of(chip * 4 * piece + cc * 2 * piece + half * piece, 32), piece)

    def out_copy(k, cc, n):
        src = ubuf if n == n_stage else stage[n]
        return pltpu.make_async_copy(src.at[spot(k, cc)], res_hbm[n].at[group_rows(k, cc), :], out_sem.at[n, spot(k, cc)])

    def compute(j, first, count):
        four = pl.ds(first, count)
        left = ubuf[four].reshape(count * piece, ubuf.shape[2])
        for n, (start, size) in enumerate(qtiles):
            @pl.when(j == 0)
            def _():
                w_copy(n).wait()
            cols = slice(start, start + size)
            part = dot_nn(left, wq[:, cols]).astype(BF16)
            stage[0][four, :, cols] = part.reshape(count, piece, size)
        for t in range(ftiles):
            @pl.when(j == 0)
            def _():
                w_copy(len(qtiles) + 2 * t).wait()
                w_copy(len(qtiles) + 2 * t + 1).wait()
            cols = slice(t * BROAD, (t + 1) * BROAD)
            gate = dot_nn(left, wg[:, cols]).astype(BF16)
            up = dot_nn(left, wu[:, cols]).astype(BF16)
            stage[1][four, :, cols] = gate.reshape(count, piece, BROAD)
            stage[2][four, :, cols] = up.reshape(count, piece, BROAD)
            if with_hidden:
                hid = gated(gate.astype(F32), up.astype(F32)).astype(BF16)
                stage[3][four, :, cols] = hid.reshape(count, piece, BROAD)
        for n in range(n_res):
            for i in range(count):
                out_copy(first // 2 + i // 2, i % 2, n).start()

    def pass_on(k):
        ici_arrived(k)
        pair_copy(k).start()

    def step(j):
        for half in HALVES:
            @pl.when(j == half + 1)
            def _():
                pass_on(x_group(half))

                @pl.when(core == 0)
                def _():
                    fwd_copy(half).start()
                pass_on(y_group(half))

                @pl.when(core == 1)
                def _():
                    fwd_copy(half).start()
        for half in HALVES:
            pair_arrived(2 * j + half)
        compute(j, 4 * j, 4)

    loop(3, step)

    def diag_step(half):
        k = d_group(half)
        pass_on(k)
        pair_arrived(k)
        compute(k, 2 * k, 2)

    loop(2, diag_step)

    for half in HALVES:
        x_copy(half).wait_send()
        y_copy(half).wait_send()
        fwd_copy(half).wait_send()

    def drain(k):
        pair_copy(k).wait_send()
        for cc in HALVES:
            for n in range(n_res):
                out_copy(k, cc, n).wait()

    loop(8, drain)


def gather_project(x_loc, total, gain_row, w_qkv, w_gate, w_up, layer, with_hidden, with_u, tp_axis, tp_size, cid):
    rows, d_model = x_loc.shape
    seq = rows * tp_size
    piece = rows // 2
    qcols, fcols = w_qkv.shape[2], w_gate.shape[2]
    with_total = total is not None
    vmem = pl.BlockSpec(memory_space=pltpu.VMEM)
    hbm = pl.BlockSpec(memory_space=pl.ANY)
    widths = [qcols, fcols, fcols] + [fcols] * with_hidden + [d_model] * with_u
    stage_widths = widths[:3 + with_hidden]
    n_w = -(-qcols // BROAD) + 2 * (fcols // BROAD)
    dma = pltpu.SemaphoreType.DMA
    local = jax.ShapeDtypeStruct((rows, d_model), BF16)
    return pl.pallas_call(
        functools.partial(ag_body, layer, with_total, with_hidden, with_u, tp_axis),
        in_specs=[vmem] * (2 + with_total) + [hbm] * 3,
        out_specs=[vmem] * (1 + with_total) + [hbm] * len(widths),
        out_shape=[local] * (1 + with_total) + [jax.ShapeDtypeStruct((seq, w), BF16) for w in widths],
        scratch_shapes=[pltpu.VMEM((d_model, qcols), BF16), pltpu.VMEM((d_model, fcols), BF16), pltpu.VMEM((d_model, fcols), BF16), pltpu.VMEM((2 * tp_size, piece, d_model), BF16)]
        + [pltpu.VMEM((2 * tp_size, piece, w), BF16) for w in stage_widths]
        + [dma((n_w,)), dma((2,)), dma((2,)), dma((8,)), dma((2,)), dma((8,)), dma((8,)), dma((len(widths), 16))],
        compiler_params=pltpu.CompilerParams(collective_id=cid, has_side_effects=True, vmem_limit_bytes=VMEM_MAX),
        cost_estimate=pl.CostEstimate(flops=4 * seq * d_model * (qcols + 2 * fcols), bytes_accessed=40 * 2 ** 20, transcendentals=0),
        name="ag_project",
    )(*([x_loc] + ([total] if with_total else []) + [gain_row, w_qkv, w_gate, w_up]))


def solution(mesh):
    tp_size = mesh.shape['tp']
    row_spec = P(('dp', 'tp'), None)
    col_spec = P(None, None, 'tp')
    inner_spec = P(None, 'tp', None)

    def device_program(x_loc, dy_loc, norm_gain, w_qkv, w_out, w_gate, w_up, w_down):
        n_layers = w_qkv.shape[0]
        heads = w_out.shape[1] // HEAD_DIM
        hcols = heads * HEAD_DIM
        seq = x_loc.shape[0] * tp_size
        cos_tab, sin_tab = rope_tables(seq)
        gather = lambda value: lax.all_gather(value, 'tp', axis=0, tiled=True)
        saved = []
        x_cur, total = x_loc, None
        dy_parts = []
        for layer in range(n_layers):
            last = layer == n_layers - 1
            results = list(gather_project(x_cur, total, norm_gain[layer:layer + 1], w_qkv, w_gate, w_up, layer, not last, last, 'tp', tp_size, 2 * n_layers + layer))
            if total is not None:
                x_cur = results.pop(0)
            u_loc, qkv, gate, up, extra = results
            if last:
                u_parts = [extra]
            query, key, value, attn, lse, dy_part = attn_forward(qkv, cos_tab, sin_tab, heads, PushOf(dy_loc, layer, n_layers, 'tp', tp_size, 3 * n_layers + 1 + layer))
            dy_parts.append(dy_part)
            saved.append((x_cur, u_loc, query, key, value, attn, lse, gate, up))
            if not last:
                total, = matmul_reduce_scatter([attn, extra], [w_out, w_down], layer, False, 'tp', tp_size, layer)

        grads = [None] * 5
        gains = [None] * n_layers
        dy_cur = dy_loc
        for layer in reversed(range(n_layers)):
            x_sav, u_loc, query, key, value, attn, lse, gate, up = saved[layer]
            d_attn, d_gate, d_up, hidden = cotangents(dy_parts, w_out, w_down, gate, up, layer, NoPush())
            d_qkv, = attn_backward(query, d_attn, lse, key, value, cos_tab, sin_tab, heads, NoPush())
            fill_ops = (1, 2) if layer else (0, 1, 2)
            norm = [x_sav, norm_gain[layer:layer + 1], dy_cur]
            if layer == 0:
                norm.append(jnp.concatenate(gains[1:]))
            dy_cur, gains[layer], *ready = matmul_reduce_scatter([d_qkv, d_gate, d_up], [w_qkv, w_gate, w_up], layer, True, 'tp', tp_size, n_layers + layer, u_parts, norm, fill_ops, 1 if layer else n_layers)
            if layer == 0:
                grads = tail_grads(attn, hidden, dy_parts, [], ready, grads, layer, n_layers)
                continue
            dy_cur, attn = lax.optimization_barrier((dy_cur, attn))
            dy_next = gather(dy_cur)
            grads = tail_grads(attn, hidden, dy_parts, u_parts, [d_qkv] + ready, grads, layer, n_layers)
            below = list(saved[layer - 1])
            dy_next, below[1], *grads = lax.optimization_barrier((dy_next, below[1], *grads))
            saved[layer - 1] = below
            u_parts = [gather(below[1])]
            dy_parts = [dy_next]
        return (dy_cur, gains[0], *grads)

    return jax.shard_map(device_program, mesh=mesh, in_specs=(row_spec, row_spec, P(None, None), col_spec, inner_spec, col_spec, col_spec, inner_spec), out_specs=(row_spec, P('dp', None), P('dp', None, 'tp'), P('dp', 'tp', None), P('dp', None, 'tp'), P('dp', None, 'tp'), P('dp', 'tp', None)), check_vma=False)
```

```python
import functools

import jax
import jax.numpy as jnp
import numpy as np
from jax import lax
from jax.experimental import pallas as pl
from jax.experimental.pallas import tpu as pltpu
from jax.sharding import PartitionSpec as P

HEAD_DIM = 128
NORM_EPS = 1e-5
ROPE_BASE = 10000.0
BF16 = jnp.bfloat16
F32 = jnp.float32
VMEM_MAX = 67043328


DIAG, XSIDE, YSIDE, SELF = range(4)
HALVES = range(2)
WHOLE = slice(None)


def loop(count, body):
    def step(i, carry):
        body(i)
        return carry

    lax.fori_loop(0, count, step, 0)


def take(refs, count):
    return [next(refs) for _ in range(count)]


def tile_ds(index, size):
    return pl.ds(pl.multiple_of(index * size, size), size)


def rope_tables(seq_len, fine=64):
    half_dim = HEAD_DIM // 2
    freqs = ROPE_BASE ** (-2.0 * np.arange(half_dim) / HEAD_DIM)

    def small(positions):
        angles = positions[:, None] * freqs[None, :]
        cos, sin = np.cos(angles), np.sin(angles)
        tables = np.concatenate([cos, cos], axis=1), np.concatenate([-sin, sin], axis=1)
        return [jnp.asarray(table.astype(np.float32)) for table in tables]

    parts = lax.optimization_barrier(small(np.arange(seq_len // fine) * fine) + small(np.arange(fine)))
    cos_far, sin_far = [part[:, None, :] for part in parts[:2]]
    cos_near, sin_near = [part[None, :, :] for part in parts[2:]]
    cos_tab = cos_far * cos_near - sin_far * sin_near
    sin_tab = sin_far * cos_near + cos_far * sin_near
    return cos_tab.reshape(seq_len, HEAD_DIM), sin_tab.reshape(seq_len, HEAD_DIM)


def rms_scale(x_f32, gain_row):
    inv_rms = lax.rsqrt(jnp.mean(x_f32 * x_f32, axis=-1, keepdims=True) + NORM_EPS)
    return x_f32 * inv_rms * gain_row


def gated(gate_f32, up_f32):
    return jax.nn.silu(gate_f32) * up_f32


def dot_nt(lhs, rhs):
    return lax.dot_general(lhs, rhs, (((1,), (1,)), ((), ())), preferred_element_type=F32)


def dot_tn(lhs, rhs):
    return lax.dot_general(lhs, rhs, (((0,), (0,)), ((), ())), preferred_element_type=F32)


def dot_nn(lhs, rhs):
    return lax.dot_general(lhs, rhs, (((1,), (0,)), ((), ())), preferred_element_type=F32)


def turn(values, cos_tab, sin_tab):
    return values * cos_tab + pltpu.roll(values, HEAD_DIM // 2, 1) * sin_tab


def ring_ids(tp_axis):
    me = lax.axis_index(tp_axis)
    core = lax.rem(me, 2)
    chip = me // 2
    x = lax.rem(chip, 2)
    y = chip // 2
    chips = ((1 - y) * 2 + (1 - x), y * 2 + (1 - x), (1 - y) * 2 + x, chip)
    partner = chip * 2 + (1 - core)
    dev_x = chips[1] * 2 + core
    dev_y = chips[2] * 2 + core
    near = dev_x * (1 - core) + dev_y * core
    far = dev_y * (1 - core) + dev_x * core
    return core, chips, partner, dev_x, dev_y, near, far


def greet(tp_axis, others):
    barrier = pltpu.get_barrier_semaphore()
    for other in others:
        pl.semaphore_signal(barrier, device_id={tp_axis: other}, device_id_type=pl.DeviceIdType.MESH)
    pl.semaphore_wait(barrier, len(others))


def remote_copy(tp_axis, src, dst, ssem, rsem, target):
    return pltpu.make_async_remote_copy(src_ref=src, dst_ref=dst, send_sem=ssem, recv_sem=rsem, device_id={tp_axis: target}, device_id_type=pl.DeviceIdType.MESH)


def sum_over(tp_axis, tp_size, slots, ssem, rsem):
    me = lax.axis_index(tp_axis)
    mine = slots.at[me]
    others = range(1, tp_size)

    def pushed(k):
        return remote_copy(tp_axis, mine, mine, ssem.at[k], rsem.at[k], lax.rem(me + k, tp_size))

    for k in others:
        pushed(k).start()
    for k in others:
        source = lax.rem(me + tp_size - k, tp_size)
        remote_copy(tp_axis, mine, slots.at[source], ssem.at[k], rsem.at[k], source).wait_recv()
    total = slots[0]
    for k in others:
        total = total + slots[k]
    for k in others:
        pushed(k).wait_send()
    return total


class PushGather:
    def __init__(self, tp_axis, src, dst, sems):
        self.tp_axis, self.src, self.dst = tp_axis, src, dst
        self.near_sem, self.far_sem, self.fwd_sem, self.ici_sem, self.pair_ssem, self.pair_rsem, self.own_sem = sems
        self.core, self.chips, self.partner, self.dev_x, self.dev_y, self.near, self.far = ring_ids(tp_axis)
        self.rows = src.shape[0]
        near_chip = self.chips[1] * (1 - self.core) + self.chips[2] * self.core
        far_chip = self.chips[2] * (1 - self.core) + self.chips[1] * self.core
        self.order = (self.chips[3], near_chip, far_chip, self.chips[0])

    def spot(self, chip, core):
        return self.dst.at[pl.ds(pl.multiple_of((chip * 2 + core) * self.rows, self.rows), self.rows), :]

    def remote(self, src, dst, ssem, rsem, target):
        return remote_copy(self.tp_axis, src, dst, ssem, rsem, target)

    def mine(self):
        return self.spot(self.chips[3], self.core)

    def near_copy(self):
        return self.remote(self.src, self.mine(), self.near_sem, self.ici_sem.at[1], self.near)

    def far_copy(self):
        return self.remote(self.src, self.mine(), self.far_sem, self.ici_sem.at[2], self.far)

    def fwd_copy(self):
        block = self.spot(self.order[1], self.core)
        return self.remote(block, block, self.fwd_sem, self.ici_sem.at[3], self.far)

    def pair_copy(self, k):
        block = self.spot(self.order[k], self.core)
        return self.remote(self.src if k == 0 else block, block, self.pair_ssem.at[k], self.pair_rsem.at[self.slot(k)], self.partner)

    def slot(self, k):
        return (0, 2, 1, 3)[k]

    def own_copy(self):
        return pltpu.make_async_copy(self.src, self.mine(), self.own_sem)

    def start(self):
        greet(self.tp_axis, (self.partner, self.dev_x, self.dev_y))
        self.near_copy().start()
        self.far_copy().start()
        self.pair_copy(0).start()
        self.own_copy().start()

    def ici_arrived(self, k):
        block = self.spot(self.order[k], self.core)
        self.remote(self.src, block, self.near_sem, self.ici_sem.at[k], self.near).wait_recv()

    def pass_sides(self):
        self.ici_arrived(1)
        self.fwd_copy().start()
        self.pair_copy(1).start()
        self.ici_arrived(2)
        self.pair_copy(2).start()

    def finish(self):
        self.ici_arrived(3)
        self.pair_copy(3).start()
        self.own_copy().wait()
        self.near_copy().wait_send()
        self.far_copy().wait_send()
        self.fwd_copy().wait_send()
        for k in range(4):
            self.pair_copy(k).wait_send()
            block = self.spot(self.order[k], 1 - self.core)
            self.remote(self.src, block, self.pair_ssem.at[k], self.pair_rsem.at[k], self.partner).wait_recv()


    def open(self, step):
        @pl.when(step == 0)
        def _():
            self.start()

        @pl.when(step == pl.num_programs(0) - 1)
        def _():
            self.pass_sides()

    def close(self, step):
        @pl.when(step == pl.num_programs(0) - 1)
        def _():
            self.finish()


class NoPush:
    n_refs, specs, shapes, sems, params, operands = 0, [], [], [], {}, []

    def __call__(self, src, dst, sems):
        return self

    def open(self, step):
        pass

    close = open


class PushOf:
    n_refs = 1

    def __init__(self, value, part, n_parts, tp_axis, tp_size, cid):
        self.tp_axis = tp_axis
        rows, self.width = value.shape[0], value.shape[1] // n_parts
        self.cols = slice(part * self.width, (part + 1) * self.width)
        dma = pltpu.SemaphoreType.DMA
        self.operands = [value]
        self.specs = [pl.BlockSpec(memory_space=pl.ANY)]
        self.shapes = [jax.ShapeDtypeStruct((rows * tp_size, self.width), BF16)]
        self.sems = [dma(())] * 3 + [dma((4,))] * 3 + [dma(())]
        self.params = {'collective_id': cid, 'has_side_effects': True}

    def __call__(self, src, dst, sems):
        return PushGather(self.tp_axis, src[0].at[:, self.cols], dst[0], list(sems))


def fold(values, op):
    acc = values[:, :HEAD_DIM]
    for at in range(HEAD_DIM, values.shape[1], HEAD_DIM):
        acc = op(acc, values[:, at:at + HEAD_DIM])
    return acc


def attn_fwd_body(heads, blk, push_of, qkv_ref, cos_ref, sin_ref, v_ref, dy_hbm, q_out, k_out, v_out, o_out, lse_out, dy_full, score_buf, k_rot, *sems):
    step = pl.program_id(0)
    push = push_of([dy_hbm], [dy_full], sems)
    push.open(step)
    scale = HEAD_DIM ** -0.5
    kcol = heads * HEAD_DIM
    vcol = kcol + HEAD_DIM
    cos_tab, sin_tab = cos_ref[...], sin_ref[...]
    here = tile_ds(step, blk)
    key = turn(qkv_ref[:, kcol:vcol].astype(F32), cos_tab, sin_tab).astype(BF16)
    k_rot[here, :] = key
    k_out[...] = key
    v_out[...] = qkv_ref[:, vcol:]
    parts = []
    for head in range(heads):
        cols = slice(head * HEAD_DIM, (head + 1) * HEAD_DIM)
        part = turn(qkv_ref[:, cols].astype(F32), cos_tab, sin_tab).astype(BF16)
        q_out[:, cols] = part
        parts.append(part)
    query = jnp.concatenate(parts, axis=0)
    rows = heads * blk

    diag = dot_nt(query, key) * scale
    row_id = lax.broadcasted_iota(jnp.int32, (heads, blk, blk), 1).reshape(rows, blk)
    col_id = lax.broadcasted_iota(jnp.int32, (rows, blk), 1)
    diag = jnp.where(row_id >= col_id, diag, -1e30)
    top = fold(diag, jnp.maximum)

    def first(j, top):
        there = tile_ds(j, blk)
        score = dot_nt(query, k_rot[there, :]) * scale
        score_buf[j] = score
        return jnp.maximum(top, fold(score, jnp.maximum))

    top = jnp.max(lax.fori_loop(0, step, first, top), axis=-1, keepdims=True)

    diag = jnp.exp(diag - top)
    total = fold(diag, jnp.add)

    def second(j, total):
        prob = jnp.exp(score_buf[j] - top)
        score_buf[j] = prob
        return total + fold(prob, jnp.add)

    total = jnp.sum(lax.fori_loop(0, step, second, total), axis=-1, keepdims=True)
    inv = 1.0 / total
    acc = dot_nn((diag * inv).astype(BF16), v_ref[here, :])

    def third(j, acc):
        there = tile_ds(j, blk)
        return acc + dot_nn((score_buf[j] * inv).astype(BF16), v_ref[there, :])

    acc = lax.fori_loop(0, step, third, acc)
    lse = top + jnp.log(total)
    lane = lax.broadcasted_iota(jnp.int32, (blk, HEAD_DIM), 1)
    packed = jnp.zeros((blk, HEAD_DIM), F32)
    for head in range(heads):
        rws = slice(head * blk, (head + 1) * blk)
        o_out[:, head * HEAD_DIM:(head + 1) * HEAD_DIM] = acc[rws].astype(BF16)
        packed = jnp.where(lane == head, lse[rws], packed)
    lse_out[...] = packed
    push.close(step)


def attn_forward(qkv, cos_tab, sin_tab, heads, push_of, blk=384):
    seq, width = qkv.shape
    hcols = heads * HEAD_DIM
    steps = seq // blk
    row = lambda i: (i, 0)
    flops = 4 * heads * seq * seq * HEAD_DIM // 2
    return pl.pallas_call(
        functools.partial(attn_fwd_body, heads, blk, push_of),
        grid=(steps,),
        in_specs=[pl.BlockSpec((blk, width), row), pl.BlockSpec((blk, HEAD_DIM), row), pl.BlockSpec((blk, HEAD_DIM), row), pl.BlockSpec((seq, HEAD_DIM), lambda i: (0, heads + 1))] + push_of.specs,
        out_specs=[pl.BlockSpec((blk, hcols), row), pl.BlockSpec((blk, HEAD_DIM), row), pl.BlockSpec((blk, HEAD_DIM), row), pl.BlockSpec((blk, hcols), row), pl.BlockSpec((blk, HEAD_DIM), row)] + push_of.specs,
        out_shape=[jax.ShapeDtypeStruct((seq, hcols), BF16), jax.ShapeDtypeStruct((seq, HEAD_DIM), BF16), jax.ShapeDtypeStruct((seq, HEAD_DIM), BF16), jax.ShapeDtypeStruct((seq, hcols), BF16), jax.ShapeDtypeStruct((seq, HEAD_DIM), F32)] + push_of.shapes,
        scratch_shapes=[pltpu.VMEM((steps, heads * blk, blk), F32), pltpu.VMEM((seq, HEAD_DIM), BF16)] + push_of.sems,
        compiler_params=pltpu.CompilerParams(**push_of.params, dimension_semantics=("arbitrary",), vmem_limit_bytes=VMEM_MAX),
        cost_estimate=pl.CostEstimate(flops=flops * 4, bytes_accessed=8 * 2 ** 20, transcendentals=heads * seq * seq // 2),
        name="attn_fwd",
    )(qkv, cos_tab, sin_tab, qkv, *push_of.operands)


def attn_bwd_body(heads, blk, push_of, q_ref, do_ref, lse_ref, k_ref, v_ref, cos_ref, sin_ref, *refs):
    refs = iter(refs)
    src = take(refs, push_of.n_refs)
    out_ref = next(refs)
    dst = take(refs, push_of.n_refs)
    prob_buf, dprob_buf, dk_acc, dv_acc = take(refs, 4)
    push = push_of(src, dst, refs)
    step = pl.program_id(0)
    push.open(step)
    scale = HEAD_DIM ** -0.5
    rows = heads * blk
    hcols = heads * HEAD_DIM
    here = tile_ds(step, blk)

    @pl.when(step == 0)
    def _():
        dk_acc[...] = jnp.zeros_like(dk_acc)
        dv_acc[...] = jnp.zeros_like(dv_acc)

    def heads_of(ref):
        return jnp.concatenate([ref[:, h * HEAD_DIM:(h + 1) * HEAD_DIM] for h in range(heads)], axis=0)

    query = heads_of(q_ref)
    d_out = heads_of(do_ref)
    lse = jnp.concatenate([lse_ref[:, h:h + 1] for h in range(heads)], axis=0)
    row_id = lax.broadcasted_iota(jnp.int32, (heads, blk, blk), 1).reshape(rows, blk)
    col_id = lax.broadcasted_iota(jnp.int32, (rows, blk), 1)

    def score_part(j, masked):
        there = tile_ds(j, blk)
        score = dot_nt(query, k_ref[there, :]) * scale
        if masked:
            score = jnp.where(row_id >= col_id, score, -1e30)
        prob = jnp.exp(score - lse)
        d_prob = dot_nt(d_out, v_ref[there, :]).astype(BF16)
        prob_buf[j] = prob
        dprob_buf[j] = d_prob
        dv_acc[there, :] += dot_tn(prob.astype(BF16), d_out)
        return fold(prob * d_prob.astype(F32), jnp.add)

    row_dot = score_part(step, True)
    row_dot = lax.fori_loop(0, step, lambda j, tot: tot + score_part(j, False), row_dot)
    row_dot = jnp.sum(row_dot, axis=-1, keepdims=True)

    def grad_part(j, acc):
        there = tile_ds(j, blk)
        d_score = (prob_buf[j] * (dprob_buf[j].astype(F32) - row_dot) * scale).astype(BF16)
        dk_acc[there, :] += dot_tn(d_score, query)
        return acc + dot_nn(d_score, k_ref[there, :])

    d_query = lax.fori_loop(0, step + 1, grad_part, jnp.zeros((rows, HEAD_DIM), F32))
    cos_tab, sin_tab = cos_ref[here, :], sin_ref[here, :]
    for head in range(heads):
        part = d_query[head * blk:(head + 1) * blk].astype(BF16).astype(F32)
        out_ref[here, head * HEAD_DIM:(head + 1) * HEAD_DIM] = turn(part, cos_tab, -sin_tab).astype(BF16)

    @pl.when(step == pl.num_programs(0) - 1)
    def _():
        d_key = dk_acc[...].astype(BF16).astype(F32)
        out_ref[:, hcols:hcols + HEAD_DIM] = turn(d_key, cos_ref[...], -sin_ref[...]).astype(BF16)
        out_ref[:, hcols + HEAD_DIM:] = dv_acc[...].astype(BF16)

    push.close(step)


def attn_backward(query, d_attn, lse, key, value, cos_tab, sin_tab, heads, push_of, blk=384):
    seq = query.shape[0]
    hcols = heads * HEAD_DIM
    width = hcols + 2 * HEAD_DIM
    steps = seq // blk
    row = lambda i: (i, 0)
    whole = lambda i: (0, 0)
    flops = 10 * heads * seq * seq * HEAD_DIM // 2
    return pl.pallas_call(
        functools.partial(attn_bwd_body, heads, blk, push_of),
        grid=(steps,),
        in_specs=[pl.BlockSpec((blk, hcols), row), pl.BlockSpec((blk, hcols), row), pl.BlockSpec((blk, HEAD_DIM), row)] + [pl.BlockSpec((seq, HEAD_DIM), whole)] * 4 + push_of.specs,
        out_specs=[pl.BlockSpec((seq, width), whole)] + push_of.specs,
        out_shape=[jax.ShapeDtypeStruct((seq, width), BF16)] + push_of.shapes,
        scratch_shapes=[pltpu.VMEM((steps, heads * blk, blk), F32), pltpu.VMEM((steps, heads * blk, blk), BF16), pltpu.VMEM((seq, HEAD_DIM), F32), pltpu.VMEM((seq, HEAD_DIM), F32)] + push_of.sems,
        compiler_params=pltpu.CompilerParams(**push_of.params, dimension_semantics=("arbitrary",), vmem_limit_bytes=VMEM_MAX),
        cost_estimate=pl.CostEstimate(flops=flops * 4, bytes_accessed=10 * 2 ** 20, transcendentals=heads * seq * seq // 2),
        name="attn_bwd",
    )(query, d_attn, lse, key, value, cos_tab, sin_tab, *push_of.operands)


def dgrad_body(n_parts, push_of, *refs):
    refs = iter(refs)
    parts = take(refs, n_parts)
    wo_ref, wd_ref, gate_ref, up_ref = take(refs, 4)
    src = take(refs, push_of.n_refs)
    dattn_ref, dgate_ref, dup_ref, hid_ref = take(refs, 4)
    push = push_of(src, take(refs, push_of.n_refs), refs)
    push.open(pl.program_id(0))

    def product(w_ref, rows):
        acc, at = None, 0
        for part in parts:
            width = part.shape[1]
            term = dot_nt(part[...], w_ref[0, rows, at:at + width])
            acc = term if acc is None else acc + term
            at += width
        return acc.astype(BF16)

    dattn_ref[...] = product(wo_ref, slice(None))
    for t in range(gate_ref.shape[1] // BROAD):
        cols = slice(t * BROAD, (t + 1) * BROAD)
        d_hidden = product(wd_ref, cols)
        hidden, pull = jax.vjp(gated, gate_ref[:, cols].astype(F32), up_ref[:, cols].astype(F32))
        d_gate, d_up = pull(d_hidden.astype(F32))
        hid_ref[:, cols] = hidden.astype(BF16)
        dgate_ref[:, cols] = d_gate.astype(BF16)
        dup_ref[:, cols] = d_up.astype(BF16)
    push.close(pl.program_id(0))


def cotangents(dy_parts, w_out, w_down, gate, up, layer, push_of, blk=512):
    seq, fcols = gate.shape
    hcols, d_model = w_out.shape[1:]
    row = lambda i: (i, 0)
    flops = 2 * seq * d_model * (hcols + fcols)
    wide = pl.BlockSpec((blk, fcols), row)
    return pl.pallas_call(
        functools.partial(dgrad_body, len(dy_parts), push_of),
        grid=(seq // blk,),
        in_specs=[pl.BlockSpec((blk, part.shape[1]), row) for part in dy_parts] + [pl.BlockSpec((1, hcols, d_model), lambda i: (layer, 0, 0)), pl.BlockSpec((1, fcols, d_model), lambda i: (layer, 0, 0)), wide, wide] + push_of.specs,
        out_specs=[pl.BlockSpec((blk, hcols), row), wide, wide, wide] + push_of.specs,
        out_shape=[jax.ShapeDtypeStruct((seq, hcols), BF16)] + [jax.ShapeDtypeStruct((seq, fcols), BF16)] * 3 + push_of.shapes,
        scratch_shapes=push_of.sems,
        compiler_params=pltpu.CompilerParams(**push_of.params, dimension_semantics=("arbitrary",), vmem_limit_bytes=VMEM_MAX),
        cost_estimate=pl.CostEstimate(flops=flops, bytes_accessed=32 * 2 ** 20, transcendentals=seq * fcols),
        name="cotangents",
    )(*dy_parts, w_out, w_down, gate, up, *push_of.operands)


def spans(parts, blk):
    result, begin = [], 0
    for part in parts:
        end = begin + part.shape[1] // blk
        result.append((begin, end - 1))
        begin = end
    return result


def on_part(step, ranges, parts, body):
    for (begin, last), part in zip(ranges, parts):
        @pl.when(jnp.logical_and(step >= begin, step <= last))
        def _():
            body(part[...])


def tail_body(dy_spans, u_spans, *refs):
    refs = iter(refs)
    attn_ref, hid_ref = take(refs, 2)
    parts = take(refs, len(dy_spans))
    u_parts = take(refs, len(u_spans))
    q_ref, g_ref, u_ref = take(refs, 3)
    q_out, out_out, g_out, u_out, down_out, right_buf = list(refs)[-6:]
    step = pl.program_id(0)

    def pick(right):
        right_buf[...] = right

    def from_dy(right):
        out_out[0] = dot_tn(attn_ref[...], right).astype(BF16)
        down_out[0] = dot_tn(hid_ref[...], right).astype(BF16)

    def from_u(left):
        q_out[0] = dot_tn(left, q_ref[...]).astype(BF16)

    if len(dy_spans) > 1:
        on_part(step, dy_spans, parts, pick)
        from_dy(right_buf[...])
    else:
        from_dy(parts[0][...])
    if u_spans:
        on_part(step, u_spans, u_parts, from_u)
    else:
        q_out[0] = q_ref[...]
    g_out[0] = g_ref[...]
    u_out[0] = u_ref[...]


def tail_grads(attn, hidden, dy_parts, u_parts, ready, grads, layer, n_layers, blk=512):
    seq = attn.shape[0]
    d_model = sum(part.shape[1] for part in dy_parts)
    whole = lambda j: (0, 0)
    hbm = pl.BlockSpec(memory_space=pl.ANY)
    rows = lambda width: pl.BlockSpec((blk, width), lambda j: (j, 0))
    rows_out = lambda width: pl.BlockSpec((1, blk, width), lambda j: (layer, j, 0))
    cols_out = lambda height: pl.BlockSpec((1, height, blk), lambda j: (layer, 0, j))

    dy_spans, u_spans = spans(dy_parts, blk), spans(u_parts, blk)

    def part_specs(ranges):
        return [pl.BlockSpec((seq, blk), lambda j, begin=begin, last=last: (0, jnp.clip(j, begin, last) - begin)) for begin, last in ranges]

    hcols, fcols = attn.shape[1], hidden.shape[1]
    widths = [item.shape[1] for item in ready]
    old = [item for item in grads if item is not None]
    before = 5 + len(dy_parts) + len(u_parts)
    q_spec = pl.BlockSpec((seq, widths[0]), whole) if u_parts else rows(widths[0])
    return pl.pallas_call(
        functools.partial(tail_body, dy_spans, u_spans),
        grid=(d_model // blk,),
        in_specs=[pl.BlockSpec((seq, hcols), whole), pl.BlockSpec((seq, fcols), whole)] + part_specs(dy_spans + u_spans) + [q_spec] + [rows(w) for w in widths[1:]] + [hbm] * len(old),
        out_specs=[rows_out(widths[0]), cols_out(hcols), rows_out(widths[1]), rows_out(widths[2]), cols_out(fcols)],
        out_shape=[jax.ShapeDtypeStruct((n_layers,) + dims, BF16) for dims in ((d_model, widths[0]), (hcols, d_model), (d_model, widths[1]), (d_model, widths[2]), (fcols, d_model))],
        input_output_aliases={before + n: n for n in range(len(old))},
        scratch_shapes=[pltpu.VMEM((seq, blk), BF16)],
        compiler_params=pltpu.CompilerParams(dimension_semantics=("arbitrary",), vmem_limit_bytes=VMEM_MAX),
        cost_estimate=pl.CostEstimate(flops=2 * seq * d_model * (hcols + fcols), bytes_accessed=60 * 2 ** 20, transcendentals=0),
        name="tail_grads",
    )(attn, hidden, *dy_parts, *u_parts, *ready, *old)


TILE = 256
WIDE = 512
BROAD = 1024
NORM_ROWS = 32


def fill_weight_grads(fill_ops, u_parts, grads, lhs, rhs, sems):
    load_sem, store_sem = sems
    seq = u_parts[0].shape[0]

    def rows_at(base, slot):
        return pl.ds(pl.multiple_of(base + slot * TILE, TILE), TILE)

    def spots(slot):
        places = (rhs[0].at[rows_at(seq, slot), :], rhs[1].at[rows_at(seq, slot), :], rhs[1].at[rows_at(seq + WIDE, slot), :])
        return [places[i] for i in fill_ops]

    def one_part(begin, steps, u_hbm):
        def load(j, slot):
            return pltpu.make_async_copy(u_hbm.at[:, tile_ds(j, TILE)], rhs[2].at[0:seq, tile_ds(slot, TILE)], load_sem.at[slot])

        def stores(j, slot):
            return [pltpu.make_async_copy(src, dst.at[tile_ds(begin + j, TILE), :], store_sem.at[slot, k]) for k, (src, dst) in enumerate(zip(spots(slot), grads))]

        load(0, 0).start()

        def step(j):
            slot = lax.rem(j, 2)
            load(j, slot).wait()

            @pl.when(j + 1 < steps)
            def _():
                load(j + 1, 1 - slot).start()

            @pl.when(j >= 2)
            def _():
                for copy in stores(j - 2, slot):
                    copy.wait()
            left = rhs[2][0:seq, tile_ds(slot, TILE)]
            for spot, i in zip(spots(slot), fill_ops):
                spot[...] = dot_tn(left, lhs[i][...]).astype(BF16)
            for copy in stores(j, slot):
                copy.start()

        loop(steps, step)
        for j in (steps - 2, steps - 1):
            for copy in stores(j, j % 2):
                copy.wait()

    begin = 0
    for u_hbm in u_parts:
        steps = u_hbm.shape[1] // TILE
        one_part(begin, steps, u_hbm)
        begin += steps


def rs_body(n_ops, layer, trans, back, fill_ops, tp_size, tp_axis, *refs):
    refs = iter(refs)
    lhs_hbm = take(refs, n_ops)
    rhs_hbm = take(refs, n_ops)
    if back:
        u_hbm = take(refs, back)
        x_ref, gain_ref, dy_ref = take(refs, 3)
        if tp_size:
            above_ref = next(refs)
        dy_out, gain_out = take(refs, 2)
        grad_hbm = take(refs, len(fill_ops))
    out_ref = next(refs)
    lhs = take(refs, n_ops)
    rhs = take(refs, n_ops)
    (own, stage, pair_in, diag_in, near_in, far_in, last_out, last_in,
     lhs_sem, rhs_sem, pair_ssem, pair_rsem, diag_ssem, diag_rsem, near_ssem, near_rsem, far_ssem, far_rsem, last_ssem, last_rsem) = take(refs, 20)
    if tp_size:
        slots, slot_ssem, slot_rsem = take(refs, 3)
    fill_sems = list(refs)
    tiles, rblk = own.shape[1:3]
    rows_out = rblk // 2
    core, chips, partner, dev_x, dev_y, near, far = ring_ids(tp_axis)
    other = 1 - core
    near_slot = XSIDE + core
    far_slot = YSIDE - core

    def row_ds(slot):
        return tile_ds(chips[slot], rblk)

    def own_ds(t):
        return tile_ds(core * tiles + t, TILE)

    def pair_ds(t):
        return tile_ds(other * tiles + t, TILE)

    def lhs_copy(i, slot):
        return pltpu.make_async_copy(lhs_hbm[i].at[row_ds(slot), :], lhs[i].at[row_ds(slot), :], lhs_sem.at[i, slot])

    def rhs_copy(i, cols, which, t):
        if trans:
            return pltpu.make_async_copy(rhs_hbm[i].at[layer, cols, :], rhs[i].at[cols, :], rhs_sem.at[i, which, t])
        return pltpu.make_async_copy(rhs_hbm[i].at[layer, :, cols], rhs[i].at[:, cols], rhs_sem.at[i, which, t])

    def pair_load(i, t):
        return rhs_copy(i, pair_ds(t), 0, t)

    def own_load(i, t):
        return rhs_copy(i, own_ds(t), 1, t)

    ops = range(n_ops)
    for i in ops:
        lhs_copy(i, DIAG).start()
    for t in range(tiles):
        for i in ops:
            pair_load(i, t).start()
        for i in ops:
            own_load(i, t).start()
    for slot in (XSIDE, YSIDE, SELF):
        for i in ops:
            lhs_copy(i, slot).start()

    if tp_size:
        me = lax.axis_index(tp_axis)
        greet(tp_axis, [lax.rem(me + k, tp_size) for k in range(1, tp_size)])
    else:
        greet(tp_axis, (partner, dev_x, dev_y))

    def product(slot, cols):
        acc = None
        for i in range(n_ops):
            left = lhs[i][row_ds(slot), :]
            part = dot_nt(left, rhs[i][cols, :]) if trans else dot_nn(left, rhs[i][:, cols])
            acc = part if acc is None else acc + part
        return acc

    remote = functools.partial(remote_copy, tp_axis)

    def spot(slot, t):
        return stage.at[t if slot in (DIAG, YSIDE) else tiles + t]

    def pair_copy(slot, t):
        return remote(spot(slot, t), pair_in.at[slot, t], pair_ssem.at[slot, t], pair_rsem.at[slot, t], partner)

    def pair_wait(slot, t):
        remote(stage.at[t], pair_in.at[slot, t], pair_ssem.at[slot, t], pair_rsem.at[slot, t], partner).wait_recv()

    def diag_copy(t):
        return remote(own.at[DIAG, t], diag_in.at[t], diag_ssem.at[t], diag_rsem.at[t], near)

    def near_copy(t):
        return remote(own.at[near_slot, t], near_in.at[t], near_ssem.at[t], near_rsem.at[t], near)

    def far_copy(t):
        return remote(own.at[far_slot, t], far_in.at[t], far_ssem.at[t], far_rsem.at[t], far)

    def last_copy(t):
        return remote(last_out.at[t], last_in.at[t], last_ssem.at[t], last_rsem.at[t], partner)

    def emit_pair(slot, t):
        spot(slot, t)[...] = product(slot, pair_ds(t))
        pair_copy(slot, t).start()

    for i in ops:
        lhs_copy(i, DIAG).wait()

    def finish_diag(t):
        pair_wait(DIAG, t)
        own[DIAG, t] += pair_in[DIAG, t]
        diag_copy(t).start()

    def lagged(finish, t):
        @pl.when(t == 0)
        def _():
            finish(t)

        @pl.when(t > 1)
        def _():
            finish(t - 1)

    def diag_step(t):
        for i in ops:
            pair_load(i, t).wait()
        emit_pair(DIAG, t)
        for i in ops:
            own_load(i, t).wait()
        own[DIAG, t] = product(DIAG, own_ds(t))
        lagged(finish_diag, t)

    loop(tiles, diag_step)
    finish_diag(tiles - 1)

    for slot in (XSIDE, YSIDE):
        for i in ops:
            lhs_copy(i, slot).wait()

    def finish_sides(t):
        pair_wait(near_slot, t)
        own[near_slot, t] += pair_in[near_slot, t]
        near_copy(t).start()
        pair_wait(far_slot, t)
        diag_copy(t).wait_recv()
        own[far_slot, t] += pair_in[far_slot, t] + diag_in[t]
        far_copy(t).start()

    def side_step(t):
        emit_pair(XSIDE, t)
        pair_copy(DIAG, t).wait_send()
        emit_pair(YSIDE, t)
        own[XSIDE, t] = product(XSIDE, own_ds(t))
        own[YSIDE, t] = product(YSIDE, own_ds(t))
        lagged(finish_sides, t)

    loop(tiles, side_step)
    finish_sides(tiles - 1)

    for i in ops:
        lhs_copy(i, SELF).wait()

    def self_step(t):
        pair_copy(XSIDE, t).wait_send()
        emit_pair(SELF, t)
        own[SELF, t] = product(SELF, own_ds(t))

    loop(tiles, self_step)

    if back:
        fill_weight_grads(fill_ops, u_hbm, grad_hbm, lhs, rhs, fill_sems)

    def final_step(t):
        pair_wait(SELF, t)
        near_copy(t).wait_recv()
        own[SELF, t] += pair_in[SELF, t] + near_in[t]
        far_copy(t).wait_recv()
        own[SELF, t] += far_in[t]
        last_out[t] = own[SELF, t, tile_ds(other, rows_out), :]
        last_copy(t).start()
        out_ref[:, own_ds(t)] = own[SELF, t, tile_ds(core, rows_out), :]

    loop(tiles, final_step)

    def close_step(t):
        last_copy(t).wait_recv()
        out_ref[:, pair_ds(t)] = last_in[t]
        for copy in (pair_copy(YSIDE, t), pair_copy(SELF, t), diag_copy(t), near_copy(t), far_copy(t), last_copy(t)):
            copy.wait_send()

    loop(tiles, close_step)

    if back:
        gain = gain_ref[...]
        gain_sum = slots.at[me, 0:1, :] if tp_size else gain_out
        gain_sum[...] = jnp.zeros_like(gain)

        def norm_step(r):
            rows = tile_ds(r, NORM_ROWS)
            pull = jax.vjp(rms_scale, x_ref[rows, :].astype(F32), gain)[1]
            d_x, d_gain = pull(out_ref[rows, :].astype(BF16).astype(F32))
            dy_out[rows, :] = (dy_ref[rows, :].astype(F32) + d_x).astype(BF16)
            gain_sum[...] += d_gain

        loop(rows_out // NORM_ROWS, norm_step)
        if tp_size:
            slots[me, 1:, :] = above_ref[...]
            gain_out[...] = sum_over(tp_axis, tp_size, slots, slot_ssem, slot_rsem)


def matmul_reduce_scatter(lhs_list, rhs_list, layer, trans, tp_axis, tp_size, cid, u_parts=(), norm=(), fill_ops=(), n_gains=1):
    n_ops = len(lhs_list)
    seq = lhs_list[0].shape[0]
    d_model = rhs_list[0].shape[1] if trans else rhs_list[0].shape[2]
    rblk = seq * 2 // tp_size
    tiles = d_model // 2 // TILE
    rows_out = seq // tp_size
    ks = [item.shape[1] for item in lhs_list]
    dma = pltpu.SemaphoreType.DMA
    scratch = [pltpu.VMEM((seq, k), BF16) for k in ks]
    scratch += [pltpu.VMEM((d_model, k) if trans else (k, d_model), BF16) for k in ks]
    scratch += [
        pltpu.VMEM((4, tiles, rblk, TILE), F32),
        pltpu.VMEM((2 * tiles, rblk, TILE), F32),
        pltpu.VMEM((4, tiles, rblk, TILE), F32),
        pltpu.VMEM((tiles, rblk, TILE), F32),
        pltpu.VMEM((tiles, rblk, TILE), F32),
        pltpu.VMEM((tiles, rblk, TILE), F32),
        pltpu.VMEM((tiles, rows_out, TILE), F32),
        pltpu.VMEM((tiles, rows_out, TILE), F32),
        dma((n_ops, 4)), dma((n_ops, 2, tiles)),
        dma((4, tiles)), dma((4, tiles)),
    ] + [dma((tiles,))] * 8
    flops = 2 * seq * d_model * sum(ks)
    hbm = pl.BlockSpec(memory_space=pl.ANY)
    vmem = pl.BlockSpec(memory_space=pltpu.VMEM)
    operands = list(lhs_list) + list(rhs_list)
    in_specs = [hbm] * len(operands)
    out_specs, out_shape = [vmem], [jax.ShapeDtypeStruct((rows_out, d_model), F32)]
    if u_parts:
        operands += u_parts + norm
        in_specs += [hbm] * len(u_parts) + [vmem] * len(norm)
        scratch = [pltpu.VMEM((rows_out, d_model), F32)] + scratch
        if n_gains > 1:
            scratch += [pltpu.VMEM((tp_size, n_gains, d_model), F32), dma((tp_size,)), dma((tp_size,))]
        scratch += [dma((2,)), dma((2, 3))]
        out_specs = [vmem] * 2 + [hbm] * len(fill_ops)
        out_shape = [jax.ShapeDtypeStruct((rows_out, d_model), BF16), jax.ShapeDtypeStruct((n_gains, d_model), F32)]
        out_shape += [jax.ShapeDtypeStruct((d_model, ks[i]), BF16) for i in fill_ops]
    return pl.pallas_call(
        functools.partial(rs_body, n_ops, layer, trans, len(u_parts), fill_ops, tp_size if n_gains > 1 else 0, tp_axis),
        in_specs=in_specs,
        out_specs=out_specs,
        out_shape=out_shape,
        scratch_shapes=scratch,
        compiler_params=pltpu.CompilerParams(collective_id=cid, has_side_effects=True, vmem_limit_bytes=VMEM_MAX),
        cost_estimate=pl.CostEstimate(flops=flops * 3, bytes_accessed=40 * 2 ** 20, transcendentals=0),
        name="matmul_rs",
    )(*operands)


def ag_body(layer, with_total, with_hidden, with_u, tp_axis, *refs):
    refs = iter(refs)
    n_stage = 3 + with_hidden
    n_res = n_stage + with_u
    x_ref = next(refs)
    if with_total:
        total_ref = next(refs)
    gain_ref, wq_hbm, wg_hbm, wu_hbm = take(refs, 4)
    if with_total:
        x_out = next(refs)
    u_out = next(refs)
    res_hbm = take(refs, n_res)
    wq, wg, wu, ubuf = take(refs, 4)
    stage = take(refs, n_stage)
    w_sem, x_ssem, y_ssem, ici_rsem, fwd_ssem, pair_ssem, pair_rsem, out_sem = refs
    piece = ubuf.shape[1]

    core, chips, partner, dev_x, dev_y, near, far = ring_ids(tp_axis)
    qcols = wq.shape[1]
    fcols = wg.shape[1]
    qtiles = [(s, min(BROAD, qcols - s)) for s in range(0, qcols, BROAD)]
    ftiles = fcols // BROAD

    def w_copy(k):
        if k < len(qtiles):
            cols = slice(qtiles[k][0], qtiles[k][0] + qtiles[k][1])
            return pltpu.make_async_copy(wq_hbm.at[layer, :, cols], wq.at[:, cols], w_sem.at[k])
        t, which = divmod(k - len(qtiles), 2)
        cols = slice(t * BROAD, (t + 1) * BROAD)
        src, dst = ((wg_hbm, wg), (wu_hbm, wu))[which]
        return pltpu.make_async_copy(src.at[layer, :, cols], dst.at[:, cols], w_sem.at[k])

    n_w = len(qtiles) + 2 * ftiles
    for k in range(n_w):
        w_copy(k).start()

    def spot(group, cc):
        return group * 2 + cc

    gain = gain_ref[...]
    for half in HALVES:
        rows = tile_ds(half, piece)
        x_f32 = x_ref[rows, :].astype(F32)
        if with_total:
            x_new = (x_f32 + total_ref[rows, :]).astype(BF16)
            x_out[rows, :] = x_new
            x_f32 = x_new.astype(F32)
        u_new = rms_scale(x_f32, gain).astype(BF16)
        u_out[rows, :] = u_new
        ubuf[spot(half, core)] = u_new
    greet(tp_axis, (partner, dev_x, dev_y))

    remote = functools.partial(remote_copy, tp_axis)

    def x_group(half):
        return 2 + 2 * half

    def y_group(half):
        return 3 + 2 * half

    def d_group(half):
        return 6 + half

    def my_piece(group):
        return ubuf.at[spot(group, core)]

    def x_copy(half):
        return remote(my_piece(half), my_piece(x_group(half)), x_ssem.at[half], ici_rsem.at[x_group(half)], dev_x)

    def y_copy(half):
        return remote(my_piece(half), my_piece(y_group(half)), y_ssem.at[half], ici_rsem.at[y_group(half)], dev_y)

    def fwd_copy(half):
        return remote(my_piece(x_group(half) + core), my_piece(d_group(half)), fwd_ssem.at[half], ici_rsem.at[d_group(half)], far)

    def pair_copy(k):
        return remote(my_piece(k), my_piece(k), pair_ssem.at[k], pair_rsem.at[k], partner)

    def pair_arrived(k):
        remote(my_piece(k), ubuf.at[spot(k, 1 - core)], pair_ssem.at[k], pair_rsem.at[k], partner).wait_recv()

    def ici_arrived(k):
        remote(my_piece(0), my_piece(k), x_ssem.at[0], ici_rsem.at[k], dev_x).wait_recv()

    for half in HALVES:
        x_copy(half).start()
        y_copy(half).start()
        pair_copy(half).start()

    def group_rows(k, cc):
        side = lax.rem(k, 2)
        is_own = (k < 2).astype(jnp.int32)
        is_diag = (k >= 6).astype(jnp.int32)
        is_side = 1 - is_own - is_diag
        side_chip = chips[1] * (1 - side) + chips[2] * side
        chip = chips[3] * is_own + chips[0] * is_diag + side_chip * is_side
        half = side * (1 - is_side) + ((k - 2) // 2) * is_side
        return pl.ds(pl.multiple_of(chip * 4 * piece + cc * 2 * piece + half * piece, 32), piece)

    def out_copy(k, cc, n):
        src = ubuf if n == n_stage else stage[n]
        return pltpu.make_async_copy(src.at[spot(k, cc)], res_hbm[n].at[group_rows(k, cc), :], out_sem.at[n, spot(k, cc)])

    def compute(j, first, count):
        four = pl.ds(first, count)
        left = ubuf[four].reshape(count * piece, ubuf.shape[2])
        for n, (start, size) in enumerate(qtiles):
            @pl.when(j == 0)
            def _():
                w_copy(n).wait()
            cols = slice(start, start + size)
            part = dot_nn(left, wq[:, cols]).astype(BF16)
            stage[0][four, :, cols] = part.reshape(count, piece, size)
        for t in range(ftiles):
            @pl.when(j == 0)
            def _():
                w_copy(len(qtiles) + 2 * t).wait()
                w_copy(len(qtiles) + 2 * t + 1).wait()
            cols = slice(t * BROAD, (t + 1) * BROAD)
            gate = dot_nn(left, wg[:, cols]).astype(BF16)
            up = dot_nn(left, wu[:, cols]).astype(BF16)
            stage[1][four, :, cols] = gate.reshape(count, piece, BROAD)
            stage[2][four, :, cols] = up.reshape(count, piece, BROAD)
            if with_hidden:
                hid = gated(gate.astype(F32), up.astype(F32)).astype(BF16)
                stage[3][four, :, cols] = hid.reshape(count, piece, BROAD)
        for n in range(n_res):
            for i in range(count):
                out_copy(first // 2 + i // 2, i % 2, n).start()

    def pass_on(k):
        ici_arrived(k)
        pair_copy(k).start()

    def step(j):
        for half in HALVES:
            @pl.when(j == half + 1)
            def _():
                pass_on(x_group(half))

                @pl.when(core == 0)
                def _():
                    fwd_copy(half).start()
                pass_on(y_group(half))

                @pl.when(core == 1)
                def _():
                    fwd_copy(half).start()
        for half in HALVES:
            pair_arrived(2 * j + half)
        compute(j, 4 * j, 4)

    loop(3, step)

    def diag_step(half):
        k = d_group(half)
        pass_on(k)
        pair_arrived(k)
        compute(k, 2 * k, 2)

    loop(2, diag_step)

    for half in HALVES:
        x_copy(half).wait_send()
        y_copy(half).wait_send()
        fwd_copy(half).wait_send()

    def drain(k):
        pair_copy(k).wait_send()
        for cc in HALVES:
            for n in range(n_res):
                out_copy(k, cc, n).wait()

    loop(8, drain)


def gather_project(x_loc, total, gain_row, w_qkv, w_gate, w_up, layer, with_hidden, with_u, tp_axis, tp_size, cid):
    rows, d_model = x_loc.shape
    seq = rows * tp_size
    piece = rows // 2
    qcols, fcols = w_qkv.shape[2], w_gate.shape[2]
    with_total = total is not None
    vmem = pl.BlockSpec(memory_space=pltpu.VMEM)
    hbm = pl.BlockSpec(memory_space=pl.ANY)
    widths = [qcols, fcols, fcols] + [fcols] * with_hidden + [d_model] * with_u
    stage_widths = widths[:3 + with_hidden]
    n_w = -(-qcols // BROAD) + 2 * (fcols // BROAD)
    dma = pltpu.SemaphoreType.DMA
    local = jax.ShapeDtypeStruct((rows, d_model), BF16)
    return pl.pallas_call(
        functools.partial(ag_body, layer, with_total, with_hidden, with_u, tp_axis),
        in_specs=[vmem] * (2 + with_total) + [hbm] * 3,
        out_specs=[vmem] * (1 + with_total) + [hbm] * len(widths),
        out_shape=[local] * (1 + with_total) + [jax.ShapeDtypeStruct((seq, w), BF16) for w in widths],
        scratch_shapes=[pltpu.VMEM((d_model, qcols), BF16), pltpu.VMEM((d_model, fcols), BF16), pltpu.VMEM((d_model, fcols), BF16), pltpu.VMEM((2 * tp_size, piece, d_model), BF16)]
        + [pltpu.VMEM((2 * tp_size, piece, w), BF16) for w in stage_widths]
        + [dma((n_w,)), dma((2,)), dma((2,)), dma((8,)), dma((2,)), dma((8,)), dma((8,)), dma((len(widths), 16))],
        compiler_params=pltpu.CompilerParams(collective_id=cid, has_side_effects=True, vmem_limit_bytes=VMEM_MAX),
        cost_estimate=pl.CostEstimate(flops=4 * seq * d_model * (qcols + 2 * fcols), bytes_accessed=40 * 2 ** 20, transcendentals=0),
        name="ag_project",
    )(*([x_loc] + ([total] if with_total else []) + [gain_row, w_qkv, w_gate, w_up]))


def solution(mesh):
    tp_size = mesh.shape['tp']
    row_spec = P(('dp', 'tp'), None)
    col_spec = P(None, None, 'tp')
    inner_spec = P(None, 'tp', None)

    def device_program(x_loc, dy_loc, norm_gain, w_qkv, w_out, w_gate, w_up, w_down):
        n_layers = w_qkv.shape[0]
        heads = w_out.shape[1] // HEAD_DIM
        hcols = heads * HEAD_DIM
        seq = x_loc.shape[0] * tp_size
        cos_tab, sin_tab = rope_tables(seq)
        gather = lambda value: lax.all_gather(value, 'tp', axis=0, tiled=True)
        saved = []
        x_cur, total = x_loc, None
        dy_parts = []
        for layer in range(n_layers):
            last = layer == n_layers - 1
            results = list(gather_project(x_cur, total, norm_gain[layer:layer + 1], w_qkv, w_gate, w_up, layer, not last, last, 'tp', tp_size, 2 * n_layers + layer))
            if total is not None:
                x_cur = results.pop(0)
            u_loc, qkv, gate, up, extra = results
            if last:
                u_parts = [extra]
            query, key, value, attn, lse, dy_part = attn_forward(qkv, cos_tab, sin_tab, heads, PushOf(dy_loc, layer, n_layers, 'tp', tp_size, 3 * n_layers + 1 + layer))
            dy_parts.append(dy_part)
            saved.append((x_cur, u_loc, query, key, value, attn, lse, gate, up))
            if not last:
                total, = matmul_reduce_scatter([attn, extra], [w_out, w_down], layer, False, 'tp', tp_size, layer)

        grads = [None] * 5
        gains = [None] * n_layers
        dy_cur = dy_loc
        for layer in reversed(range(n_layers)):
            x_sav, u_loc, query, key, value, attn, lse, gate, up = saved[layer]
            d_attn, d_gate, d_up, hidden = cotangents(dy_parts, w_out, w_down, gate, up, layer, NoPush())
            d_qkv, = attn_backward(query, d_attn, lse, key, value, cos_tab, sin_tab, heads, NoPush())
            fill_ops = (1, 2) if layer else (0, 1, 2)
            norm = [x_sav, norm_gain[layer:layer + 1], dy_cur]
            if layer == 0:
                norm.append(jnp.concatenate(gains[1:]))
            dy_cur, gains[layer], *ready = matmul_reduce_scatter([d_qkv, d_gate, d_up], [w_qkv, w_gate, w_up], layer, True, 'tp', tp_size, n_layers + layer, u_parts, norm, fill_ops, 1 if layer else n_layers)
            if layer == 0:
                grads = tail_grads(attn, hidden, dy_parts, [], ready, grads, layer, n_layers)
                continue
            dy_cur, attn = lax.optimization_barrier((dy_cur, attn))
            dy_next = gather(dy_cur)
            grads = tail_grads(attn, hidden, dy_parts, u_parts, [d_qkv] + ready, grads, layer, n_layers)
            below = list(saved[layer - 1])
            dy_next, below[1], *grads = lax.optimization_barrier((dy_next, below[1], *grads))
            saved[layer - 1] = below
            u_parts = [gather(below[1])]
            dy_parts = [dy_next]
        return (dy_cur, gains[0], *grads)

    return jax.shard_map(device_program, mesh=mesh, in_specs=(row_spec, row_spec, P(None, None), col_spec, inner_spec, col_spec, col_spec, inner_spec), out_specs=(row_spec, P('dp', None), P('dp', None, 'tp'), P('dp', 'tp', None), P('dp', None, 'tp'), P('dp', None, 'tp'), P('dp', 'tp', None)), check_vma=False)
```
